32 devices in a mesh: gx: 4 (over z), gy: 4 (over x, core), gz: 2 (over y).
Axes of the slice: x: 2, y: 2, z: 4, core: 2. Of those that a mesh axis runs over, the one named last changes fastest.
Arguments:
- charges: bfloat16 [256, 256, 256], P('gx', 'gy', 'gz'), may hold values from -6 to 6
- taps: float32 [4, 4, 17], replicated, may hold values from 0.05 to 0.3
Outputs:
- potential: bfloat16 [256, 256, 256], P('gx', 'gy', 'gz')
The draws below stay inside these ranges and needn't reach their ends.
All inputs are finite; a program needn't handle non-finite values.
Results may differ from the reference program's by a relative error of at most 0.012.
The reference program's roundings to bfloat16 on the way (of `section`) count: a program that leaves them out, or rounds other values in their place, can miss the bound.
Values may be sent and summed in bfloat16 or wider, within the bound.
No kernel may reach another device: no remote copies, remote signals or barrier semaphores. Data moves between devices by JAX's collectives and lax.ppermute only.
A program may use at most 128 MiB of HBM per device.

```python
import jax
import jax.numpy as jnp
from jax import lax

TERMS = 4
TAPS = 17
LEVELS = 4
NX = 256
NY = 256
NZ = 256


def draw_charges(key, part):
    shape = (NX, NY, NZ)
    first_key = jax.random.fold_in(key, 0)
    field = jax.random.normal(first_key, shape, jnp.float32)
    total = 6.0 * field
    for along in range(3):
        total = total - jnp.roll(field, 1, along) - jnp.roll(field, -1, along)
    return jnp.clip(0.15 * total, -6.0, 6.0).astype(jnp.bfloat16)


def setup_inputs(seed: int = 0) -> dict:
    streams_of = jax.random.split(jax.random.key(seed), 3)
    charges = draw_charges(jax.random.fold_in(streams_of[2], 71), 0)
    taps = jnp.clip(jax.random.uniform(streams_of[1], (LEVELS, TERMS, TAPS), jnp.float32, 0.05, 0.3), 0.05, 0.3)
    return dict(charges=charges, taps=taps)


def restrict_padded(padded):
    for along in range(3):
        fine_count = padded.shape[along] - 6

        def strided(offset):
            return lax.slice_in_dim(padded, 3 + offset, 3 + offset + fine_count, 2, along)

        padded = (16.0 * strided(0) + 9.0 * (strided(-1) + strided(1)) - (strided(-3) + strided(3))) / 16.0
    return padded


def prolong_padded(padded):
    for along in range(3):
        coarse_count = padded.shape[along] - 4

        def shifted(start):
            return lax.slice_in_dim(padded, start, start + coarse_count, 1, along)

        centre = shifted(2)
        between = (9.0 * (centre + shifted(3)) - (shifted(1) + shifted(4))) / 16.0
        shape_list = list(centre.shape)
        shape_list[along] = 2 * coarse_count
        padded = jnp.stack([centre, between], along + 1).reshape(shape_list)
    return padded


def restrict(field):
    return restrict_padded(jnp.pad(field, 3, mode="wrap"))


def prolong(field):
    return prolong_padded(jnp.pad(field, 2, mode="wrap"))


def shifted_sum(padded, tap_row, along, length):
    total = jnp.zeros(padded.shape[:along] + (length,) + padded.shape[along + 1:], jnp.float32)
    for offset in range(tap_row.shape[0]):
        total = total + tap_row[offset] * lax.slice_in_dim(padded, offset, offset + length, 1, along)
    return total


def rounded(values):
    return lax.optimization_barrier(values.astype(jnp.bfloat16)).astype(jnp.float32)


def kernel_level(field, level_taps):
    charged = rounded(field)
    factors = rounded(level_taps)
    padded = jnp.pad(charged, 8, mode="wrap")
    potential = jnp.zeros(field.shape, jnp.float32)
    for term in range(factors.shape[0]):
        section = rounded(shifted_sum(padded, factors[term], 2, field.shape[2]))
        section = rounded(shifted_sum(section, factors[term], 1, field.shape[1]))
        section = shifted_sum(section, factors[term], 0, field.shape[0])
        potential = potential + section
    return potential


def reference(charges, taps):
    level_zero = charges.astype(jnp.float32)
    level_one = restrict(level_zero)
    level_two = restrict(level_one)
    level_three = restrict(level_two)
    kernel_zero = kernel_level(level_zero, taps[0])
    kernel_one = kernel_level(level_one, taps[1])
    kernel_two = kernel_level(level_two, taps[2])
    kernel_three = kernel_level(level_three, taps[3])
    potential_two = kernel_two + prolong(kernel_three)
    potential_one = kernel_one + prolong(potential_two)
    potential_zero = kernel_zero + prolong(potential_one)
    return potential_zero.astype(jnp.bfloat16)
```

```python
import functools

import jax
import jax.numpy as jnp
import numpy as np
from jax import lax
from jax.experimental import pallas as pl
from jax.experimental.pallas import tpu as pltpu
from jax.sharding import PartitionSpec as P

F32, BF16 = jnp.float32, jnp.bfloat16
REACH = 8
LANES = 128
TILE = 16
SLAB = 16
LOW, HIGH = (0, 1, 2, 2), (0, 2, 3, 3)
STENCIL = ((0, 1.0), (-1, 9 / 16), (1, 9 / 16), (-3, -1 / 16), (3, -1 / 16))


def up_to(value, step):
    return -(-value // step) * step


class Level:
    def __init__(self, index, block):
        self.index = index
        self.n = tuple(size >> index for size in block)
        self.low, self.high = LOW[index], HIGH[index]
        self.win = tuple(size + self.low + self.high for size in self.n)
        self.full = tuple(size + 2 * REACH for size in self.win)
        self.out = tuple(up_to(size, TILE) for size in self.win[:2])
        self.inp = tuple(size + TILE for size in self.out)
        self.rows = up_to(self.win[1], 8)
        self.lane = 0
        self.start = 0
        self.span = up_to(self.full[0] * self.inp[1], LANES)


def levels_of(block):
    levels = [Level(index, block) for index in range(4)]
    lane, start = 0, 0
    for level in levels[1:]:
        level.lane, level.start = lane, start
        lane += level.win[2]
        start += level.span
    assert lane <= LANES and block[2] == LANES
    assert all(level.n[d] % 8 == 0 for level in levels for d in range(3))
    return levels


def own_lane(level, z):
    return (level.lane + z + level.low + REACH) % LANES


def restrict_rows(coarse, fine):
    fine_rows = fine.n[1] if fine.index == 0 else fine.rows
    matrix = np.zeros((coarse.rows, 2, fine_rows))
    for row in range(coarse.win[1]):
        for offset, weight in STENCIL:
            col = 2 * (row - coarse.low) + offset + fine.low
            if 0 <= col < fine.win[1]:
                matrix[row, :, col] = weight
    return matrix.reshape(coarse.rows, 2 * fine_rows)


def restrict_lanes(coarse, fine):
    matrix = np.zeros((2, LANES, LANES))
    for z in range(-coarse.low, coarse.n[2] + coarse.high):
        for offset, weight in STENCIL:
            at = 2 * z + offset
            if -fine.low <= at < fine.n[2] + fine.high:
                lane = at if fine.index == 0 else own_lane(fine, at)
                matrix[:, lane, own_lane(coarse, z)] = weight
    return matrix.reshape(2 * LANES, LANES)


def prolong_weights(fine_at):
    half = fine_at // 2
    if fine_at % 2 == 0:
        return ((half, 1.0),)
    return ((half, 9 / 16), (half + 1, 9 / 16), (half - 1, -1 / 16), (half + 2, -1 / 16))


def prolong_matrix(fine_count, fine_win, fine_low, coarse_count, coarse_low):
    matrix = np.zeros((fine_count, coarse_count))
    for row in range(fine_win):
        for at, weight in prolong_weights(row - fine_low):
            if 0 <= at + coarse_low < coarse_count:
                matrix[row, at + coarse_low] = weight
    return matrix


def prolong_rows(fine, coarse):
    matrix = prolong_matrix(fine.out[1], fine.win[1], fine.low, coarse.out[1], coarse.low)
    return np.concatenate([matrix, matrix], 1)


def prolong_lanes(fine, coarse):
    matrix = prolong_matrix(LANES, fine.win[2], fine.low, LANES, coarse.low).T
    return np.concatenate([matrix, matrix], 0)


def send_lanes(level):
    up, down = np.zeros((SLAB, LANES)), np.zeros((SLAB, LANES))
    for j in range(SLAB):
        s = level.n[2] - REACH + j
        if s < level.win[2]:
            up[j, own_lane(level, s - level.low)] = 1
        if j < level.low + level.high + REACH:
            down[j, own_lane(level, j - level.low)] = 1
    return np.concatenate([up, down], 0)


def place_lanes(level):
    from_prev, from_next = np.zeros((SLAB, LANES)), np.zeros((SLAB, LANES))
    for j in range(SLAB):
        if level.n[2] - REACH + j < level.win[2]:
            from_prev[j, (level.lane + j) % LANES] = 1
        at = j + REACH + level.n[2]
        if at < level.full[2]:
            from_next[j, (level.lane + at) % LANES] = 1
    return np.concatenate([from_prev, from_next] * (1 if level.index == 1 else 2), 0)


def dot(a, b, dims=((1,), (0,))):
    return lax.dot_general(a, b, (dims, ((), ())), preferred_element_type=F32)


def split_rows(x):
    high = x.astype(BF16).astype(F32)
    return jnp.concatenate([high, x - high], 0).astype(BF16)


def split_lanes(x):
    high = x.astype(BF16).astype(F32)
    return jnp.concatenate([high, x - high], 1).astype(BF16)


class Table:
    def __init__(self):
        self.parts, self.places, self.count = [], {}, 0

    def add(self, key, matrix):
        rows, cols = matrix.shape
        padded = np.zeros((up_to(rows, TILE), LANES), np.float32)
        padded[:rows, :cols] = matrix
        self.places[key] = (self.count, rows, cols)
        self.parts.append(padded)
        self.count += padded.shape[0]

    def array(self):
        return jnp.asarray(np.concatenate(self.parts, 0), BF16)

    def get(self, ref, *key):
        start, rows, cols = self.places[key]
        return ref[start : start + rows, :cols]


def pad_rows(x, rows):
    if x.shape[0] == rows:
        return x
    return jnp.concatenate([x, jnp.zeros((rows - x.shape[0], x.shape[1]), x.dtype)], 0)


def total(terms):
    return functools.reduce(lambda a, b: a + b, terms)


def bands_kernel(levels, taps_ref, band_ref, lanes_ref):
    row = lax.broadcasted_iota(jnp.int32, (8 * TILE, 16 * TILE), 0)
    col = lax.broadcasted_iota(jnp.int32, (8 * TILE, 16 * TILE), 1)
    offset = jnp.where(row % 8 == col // 32, col % 32 - row // 8, -1)

    @pl.loop(0, 16)
    def _(which):
        matrix = jnp.zeros(offset.shape, F32)
        for tap in range(17):
            matrix = jnp.where(offset == tap, taps_ref[which, tap], matrix)
        band_ref[which] = matrix.astype(BF16)

    for level in levels:
        first, count = lane_rows(level)
        k = lax.broadcasted_iota(jnp.int32, (count, LANES), 0)
        z_out = lax.broadcasted_iota(jnp.int32, (count, LANES), 1)
        if level.index == 0:
            n = level.n[2]
            z_in = jnp.where(k < n, k + REACH, jnp.where(k < n + REACH, k - n, k))
            valid = k < n + 2 * REACH
        else:
            z_in = (k + (LANES - level.lane)) % LANES
            valid = (z_in < level.full[2]) & (z_out < level.win[2])
        offset_z = jnp.where(valid, z_in - z_out, -1)
        for term in range(4):
            matrix = jnp.zeros(offset_z.shape, F32)
            for tap in range(17):
                matrix = jnp.where(offset_z == tap, taps_ref[4 * level.index + term, tap], matrix)
            lanes_ref[first : first + count, term_lanes(term)] = matrix.astype(BF16)


def lane_rows(level):
    return (0, 2 * LANES) if level.index == 0 else ((level.index + 1) * LANES, LANES)


def term_lanes(term):
    return slice(term * LANES, (term + 1) * LANES)


def plane_at(levels, level, which, rows):
    first = 0
    for other in levels[1:]:
        sizes = (other.win[0], other.rows) if rows == "own" else (other.full[0], other.rows)
        if other is level:
            return slice(first + which * sizes[1], first + (which + 1) * sizes[1])
        first += sizes[0] * sizes[1]
    return first


def halves_of(x):
    high = x.astype(BF16).astype(F32)
    return high, x - high


def restrict_kernel(levels, table, charges_ref, table_ref, q_ref, up_ref, down_ref, far_ref):
    for level, fine in zip(levels[1:], levels[:3]):
        for at in range(level.win[0]):
            terms = {}
            for offset, weight in STENCIL:
                plane = 2 * (at - level.low) + offset + fine.low
                if 0 <= plane < fine.win[0]:
                    if fine.index == 0:
                        value = charges_ref[plane].astype(F32)
                    else:
                        value = q_ref[plane_at(levels, fine, plane, "own")]
                    terms.setdefault(weight, []).append(value)
            value = total([total(group) * weight for weight, group in terms.items()])
            value = dot(table.get(table_ref, "rows", level.index), split_rows(value))
            value = dot(split_lanes(value), table.get(table_ref, "lanes", level.index))
            q_ref[plane_at(levels, level, at, "own")] = value
    rows, rest_rows = levels[1].rows, levels[2].rows
    for j in range(up_ref.shape[0]):
        for slab_ref, bases in ((up_ref, [lv.n[0] - REACH for lv in levels[1:]]), (down_ref, [0] * 3)):
            highs, rests = [], [jnp.zeros((rest_rows, LANES), F32)]
            for level, base in zip(levels[1:], bases):
                if base + j < level.win[0]:
                    high, rest = halves_of(q_ref[plane_at(levels, level, base + j, "own")])
                    highs.append(pad_rows(high, rows))
                    if level.index > 1:
                        rests.append(pad_rows(rest, rest_rows))
            slab_ref[j] = jnp.concatenate([total(highs), total(rests)], 0).astype(BF16)
    last = levels[3]
    pack_far(
        far_ref,
        [q_ref[plane_at(levels, last, at, "own")] for at in range(last.win[0])],
    )


def pack_far(far_ref, planes):
    for group in range(far_ref.shape[0]):
        members = planes[4 * group : 4 * group + 4]
        far_ref[group] = total(
            [pltpu.roll(x, 32 * k, 1) if k else x for k, x in enumerate(members)]
        )


def unpack_far(far_ref, at):
    x = far_ref[at // 4]
    return pltpu.roll(x, LANES - 32 * (at % 4), 1) if at % 4 else x


def lane_masks(levels):
    lane = lax.broadcasted_iota(jnp.int32, (8, LANES), 1)
    masks = []
    for level in levels[1:]:
        at = (lane + (2 * LANES - level.lane - REACH)) % LANES
        masks.append((at < level.win[2])[:1])
    return masks


def rows_kernel(levels, q_ref, prev_ref, next_ref, far_prev_ref, *refs):
    far_next_ref = far_prev_ref if len(refs) == 4 else refs[0]
    x_ref, up_ref, down_ref, far_ref = refs[-4:]
    count, high_rows = prev_ref.shape[0], levels[1].rows
    masks = lane_masks(levels)
    coarsest = []

    def received(ref, at, level):
        slab = ref[at].astype(F32)
        high = slab[: level.rows]
        return high if level.index == 1 else high + slab[high_rows : high_rows + level.rows]

    rest_count = levels[2].full[0]
    for at in range(levels[1].full[0]):
        ups, downs = [], []
        for level, mask in zip(levels[1:], masks):
            if at >= level.full[0]:
                continue
            n = level.n[0]
            terms = []
            if 0 <= at - REACH < level.win[0]:
                terms.append(q_ref[plane_at(levels, level, at - REACH, "own")])
            if at < count and at - REACH + n < level.win[0]:
                terms.append(received(prev_ref, at, level))
            if 0 <= at - REACH - n < count:
                terms.append(received(next_ref, at - REACH - n, level))
            if level.index == 3:
                if at - REACH + 2 * n < level.win[0]:
                    terms.append(unpack_far(far_prev_ref, at - REACH + 2 * n))
                if at - REACH - 2 * n >= 0:
                    terms.append(unpack_far(far_next_ref, at - REACH - 2 * n))
            value = jnp.where(mask, total(terms), 0.0)
            x_ref[plane_at(levels, level, at, "full")] = value
            first = level.n[1] - REACH
            ups.append((level.index, halves_of(value[first : first + SLAB])))
            downs.append((level.index, halves_of(value[:SLAB])))
            if level.index == 3:
                coarsest.append(value)
        for slab_ref, parts in ((up_ref, ups), (down_ref, downs)):
            slab_ref[at] = total([x for _, (x, _) in parts]).astype(BF16)
            rests = [x for index, (_, x) in parts if index > 1]
            if rests:
                slab_ref[levels[1].full[0] + at] = total(rests).astype(BF16)
    pack_far(far_ref, coarsest)


def lanes_kernel(levels, table, x_ref, prev_ref, next_ref, far_prev_ref, *refs):
    far_next_ref = far_prev_ref if len(refs) == 3 else refs[0]
    table_ref, flat_ref, slab_ref = refs[-3:]

    def received(ref, at, level):
        high = ref[at].astype(F32)
        return high if level.index == 1 else high + ref[levels[1].full[0] + at].astype(F32)

    for level, mask in zip(levels[1:], lane_masks(levels)):
        blocks, step = level.inp[1] // 8, level.n[1] // 8
        for at in range(level.full[0]):
            own = x_ref[plane_at(levels, level, at, "full")]
            slabs = [received(prev_ref, at, level), received(next_ref, at, level)]
            if level.index == 3:
                slabs += [unpack_far(far_prev_ref, at), unpack_far(far_next_ref, at)]
            parts = []
            for block in range(blocks):
                terms = []
                if 0 <= block - 1 < level.rows // 8:
                    terms.append(own[8 * block - 8 : 8 * block])
                places = [block, block - 1 - step, block - 1 + 2 * step, block - 1 - 2 * step]
                for slab, place in zip(slabs, places):
                    if 0 <= place < SLAB // 8:
                        terms.append(slab[8 * place : 8 * place + 8])
                parts.append(total(terms) if terms else jnp.zeros((8, LANES), F32))
            value = jnp.where(mask, jnp.concatenate(parts, 0), 0.0)
            first = level.start + at * level.inp[1]
            flat_ref[first : first + level.inp[1]] = value
        used = level.start + level.full[0] * level.inp[1]
        last = level.start + level.span
        if used < last:
            flat_ref[used:last] = jnp.zeros((last - used, LANES), F32)
    shift = levels[-1].start + levels[-1].span - levels[2].start
    for level in levels[1:]:
        send = table.get(table_ref, "send", level.index)
        for first in range(level.start, level.start + level.span, 512):
            stop = min(first + 512, level.start + level.span)
            high, rest = halves_of(flat_ref[first:stop])
            slab_ref[:, first:stop] = dot(send, high.astype(BF16), ((1,), (1,))).astype(BF16)
            if level.index > 1:
                slab_ref[:, first + shift : stop + shift] = dot(
                    send, rest.astype(BF16), ((1,), (1,))
                ).astype(BF16)


def halo_kernel(wide_ref, out_ref):
    planes, rows, count = wide_ref.shape
    row = lax.broadcasted_iota(jnp.int32, (2 * REACH, count), 0)
    lane = lax.broadcasted_iota(jnp.int32, (2 * REACH, count), 1)
    send = jnp.where(lane == (row + (count - REACH)) % count, 1.0, 0.0).astype(BF16)
    step = 8
    for first in range(0, planes, step):
        chunk = wide_ref[first : first + step].reshape(step * rows, LANES)
        out_ref[:, first * rows : (first + step) * rows] = dot(send, chunk, ((1,), (1,))).astype(BF16)


def two_passes(level, band, first_ref, second_ref, put):
    def parts_of(result):
        parts = [result[:, :LANES], result[:, LANES:]]
        return jnp.concatenate([x.reshape(TILE, 8, LANES) for x in parts], 1)

    def along_y(pair):
        for block in range(level.out[1] // TILE):
            for term in range(4):
                halves = [
                    first_ref[
                        pl.ds(pair * 16 + 8 * half, 8),
                        TILE * block : TILE * block + 32,
                        term_lanes(term),
                    ].reshape(256, LANES)
                    for half in range(2)
                ]
                result = dot(band(term), jnp.concatenate(halves, 1))
                second_ref[
                    term, TILE * block : TILE * (block + 1), pl.ds(pl.multiple_of(pair * 16, 16), 16)
                ] = parts_of(result).astype(BF16)

    def along_x(pair):
        for block in range(level.out[0] // TILE):
            result = None
            for term in range(4):
                halves = [
                    second_ref[
                        term, pl.ds(pair * 16 + 8 * half, 8), TILE * block : TILE * block + 32
                    ].reshape(256, LANES)
                    for half in range(2)
                ]
                part = dot(band(term), jnp.concatenate(halves, 1))
                result = part if result is None else result + part
            put(block, pair, parts_of(result))

    pl.loop(0, level.inp[0] // 16)(along_y)
    pl.loop(0, level.out[1] // 16)(along_x)


def fine_kernel(level, wide_ref, halo_ref, lanes_ref, band_ref, out_ref, first_ref, second_ref):
    rows, step = level.inp[1], 8
    row = lax.broadcasted_iota(jnp.int32, (2 * REACH, LANES), 0)
    lane = lax.broadcasted_iota(jnp.int32, (2 * REACH, LANES), 1)
    place = jnp.where(lane == row, 1.0, 0.0).astype(BF16)

    @pl.loop(0, level.inp[0] // step)
    def _(chunk):
        where = pl.ds(pl.multiple_of(chunk * step * rows, LANES), step * rows)
        sides = dot(halo_ref[:, where], place, ((0,), (0,))).astype(BF16)
        here = wide_ref[pl.ds(chunk * step, step)].reshape(step * rows, LANES)
        result = dot(jnp.concatenate([here, sides], 1), lanes_ref[: 2 * LANES])
        first_ref[pl.ds(chunk * step, step)] = result.astype(BF16).reshape(step, rows, 4 * LANES)

    def put(block, pair, value):
        out_ref[TILE * block : TILE * (block + 1), pl.ds(pl.multiple_of(pair * 16, 16), 16)] = value

    two_passes(level, lambda term: band_ref[term], first_ref, second_ref, put)


def coarse_kernel(levels, table, flat_ref, slab_ref, lanes_ref, band_ref, table_ref, fine_ref, *refs):
    out_ref, first_refs, second_refs, sum_refs = refs[0], refs[1:4], refs[4:7], refs[7:10]
    shift = levels[-1].start + levels[-1].span - levels[2].start
    for level in reversed(levels[1:]):
        which = level.index - 1
        first_ref, sum_ref = first_refs[which], sum_refs[which]
        rows, step = level.inp[1], 4
        first_lane, _ = lane_rows(level)
        place = table.get(table_ref, "place", level.index)
        for plane in range(0, level.full[0], step):
            count = min(step, level.full[0] - plane)
            if (count * rows) % LANES:
                count += 1
            start, stop = level.start + plane * rows, level.start + (plane + count) * rows
            slab = slab_ref[:, start:stop]
            if level.index > 1:
                slab = jnp.concatenate([slab, slab_ref[:, start + shift : stop + shift]], 0)
            value = flat_ref[start:stop] + dot(slab, place, ((0,), (0,)))
            result = dot(value.astype(BF16), lanes_ref[first_lane : first_lane + LANES])
            first_ref[plane : plane + count] = result.astype(BF16).reshape(count, rows, 4 * LANES)
        rest = level.inp[0] - plane - count
        if rest > 0:
            first_ref[plane + count :] = jnp.zeros((rest, rows, 4 * LANES), BF16)

        def put(block, pair, value, sum_ref=sum_ref):
            sum_ref[TILE * block : TILE * (block + 1), pl.ds(pl.multiple_of(pair * 16, 16), 16)] = value

        base = 4 * level.index
        two_passes(level, lambda term, base=base: band_ref[base + term], first_ref, second_refs[which], put)

    def stretch(fine, coarse, source):
        planes, rows, _ = source.shape
        for first in range(0, coarse.win[0], 4):
            count = min(4, planes - first)
            value = split_lanes(source[first : first + count].reshape(count * rows, LANES))
            value = dot(value, table.get(table_ref, "zed", fine.index))
            source[first : first + count] = value.reshape(count, rows, LANES)

    def prolong(fine, coarse, halves, source, emit):
        planes = []
        for half in halves:
            at = half + coarse.low
            between = (9.0 * (source[at] + source[at + 1]) - (source[at - 1] + source[at + 2])) / 16.0
            planes += [split_rows(source[at]), split_rows(between)]
        both = dot(table.get(table_ref, "tall", fine.index), jnp.concatenate(planes, 1))
        for k, half in enumerate(halves):
            emit(2 * half, both[:, 2 * k * LANES : (2 * k + 1) * LANES])
            emit(2 * half + 1, both[:, (2 * k + 1) * LANES : (2 * k + 2) * LANES])

    for fine, coarse in ((levels[2], levels[3]), (levels[1], levels[2])):
        sum_ref = sum_refs[fine.index - 1]
        source = sum_refs[coarse.index - 1]
        stretch(fine, coarse, source)

        def emit(at, value, fine=fine, sum_ref=sum_ref):
            plane = at + fine.low
            if 0 <= plane < fine.win[0]:
                sum_ref[plane] = sum_ref[plane] + value

        for half in range(-1, (fine.n[0] + fine.high + 1) // 2):
            prolong(fine, coarse, [half], source, emit)

    stretch(levels[0], levels[1], sum_refs[0])

    @pl.loop(0, levels[0].n[0] // 8)
    def _(group):
        def emit(at, value):
            out_ref[at] = (fine_ref[at] + value).astype(BF16)

        prolong(levels[0], levels[1], [4 * group + k for k in range(4)], sum_refs[0], emit)


def make_table(levels):
    table = Table()
    for level, fine in zip(levels[1:], levels[:3]):
        table.add(("rows", level.index), restrict_rows(level, fine))
        table.add(("lanes", level.index), restrict_lanes(level, fine))
        table.add(("send", level.index), send_lanes(level))
        table.add(("place", level.index), place_lanes(level))
        table.add(("tall", fine.index), prolong_rows(fine, level))
        table.add(("zed", fine.index), prolong_lanes(fine, level))
    return table


def call(kernel, out_shape, args, scratch=(), smem=(), flops=0):
    specs = [
        pl.BlockSpec(memory_space=pltpu.SMEM if i in smem else pltpu.VMEM) for i in range(len(args))
    ]
    single = not isinstance(out_shape, (list, tuple))
    outs = [out_shape] if single else list(out_shape)
    out_specs = [pl.BlockSpec(memory_space=pltpu.VMEM) for _ in outs]
    return pl.pallas_call(
        kernel,
        out_shape=out_shape,
        in_specs=specs,
        out_specs=out_specs[0] if single else out_specs,
        scratch_shapes=list(scratch),
        compiler_params=pltpu.CompilerParams(vmem_limit_bytes=60000 * 1024),
        cost_estimate=pl.CostEstimate(flops=flops, bytes_accessed=1 << 20, transcendentals=0),
    )(*args)


def shape(sizes, dtype):
    return jax.ShapeDtypeStruct(tuple(sizes), dtype)


def shifted(value, axis, by):
    count = lax.axis_size(axis)
    return lax.ppermute(value, axis, [(i, (i + by) % count) for i in range(count)])


def far_pair(value, axis):
    after = shifted(value, axis, 2)
    return [after] if lax.axis_size(axis) == 4 else [after, shifted(value, axis, -2)]


def z_pair(value, axis):
    half = value.shape[0] // 2
    if lax.axis_size(axis) == 2:
        return shifted(value, axis, 1)
    return jnp.concatenate([shifted(value[:half], axis, 1), shifted(value[half:], axis, -1)], 0)


def per_device(charges, taps):
    levels = levels_of(charges.shape)
    table = make_table(levels)
    table_array = table.array()
    zero, coarse = levels[0], levels[1:]
    reach = REACH

    x_prev = shifted(charges[-reach:], "gx", 1)
    x_next = shifted(charges[:reach], "gx", -1)

    slab_planes = max(level.low + level.high + reach for level in coarse)
    slab_rows = levels[1].rows + levels[2].rows
    q, l_up, l_down, l_far = call(
        functools.partial(restrict_kernel, levels, table),
        [shape((sum(lv.win[0] * lv.rows for lv in coarse), LANES), F32)]
        + [shape((slab_planes, slab_rows, LANES), BF16)] * 2
        + [shape((up_to(levels[3].win[0], 4) // 4, SLAB, LANES), F32)],
        [charges, table_array],
        flops=1 << 27,
    )
    band, lanes = call(
        functools.partial(bands_kernel, levels),
        [shape((16, 8 * TILE, 16 * TILE), BF16), shape((5 * LANES, 4 * LANES), BF16)],
        [taps.reshape(16, 17)],
        smem=(0,),
        flops=1 << 26,
    )

    l_prev = shifted(l_up, "gx", 1)
    l_next = shifted(l_down, "gx", -1)
    far = far_pair(l_far, "gx")

    pieces = (x_prev, charges, x_next)
    y_prev = shifted(jnp.concatenate([x[:, -reach:] for x in pieces], 0), "gy", 1)
    y_next = shifted(jnp.concatenate([x[:, :reach] for x in pieces], 0), "gy", -1)

    r, m_up, m_down, m_far = call(
        functools.partial(rows_kernel, levels),
        [shape((sum(lv.full[0] * lv.rows for lv in coarse), LANES), F32)]
        + [shape((levels[1].full[0] + levels[2].full[0], SLAB, LANES), BF16)] * 2
        + [shape((up_to(levels[3].full[0], 4) // 4, SLAB, LANES), F32)],
        [q, l_prev, l_next, *far],
        flops=1 << 25,
    )
    m_prev = shifted(m_up, "gy", 1)
    m_next = shifted(m_down, "gy", -1)
    far = far_pair(m_far, "gy")

    wide = jnp.concatenate([y_prev, jnp.concatenate(pieces, 0), y_next], 1)
    sides = call(
        halo_kernel,
        shape((2 * reach, wide.shape[0] * wide.shape[1]), BF16),
        [wide],
        flops=1 << 26,
    )
    halo = z_pair(sides, "gz")

    flat_rows = sum(level.span for level in coarse)
    flat, slabs = call(
        functools.partial(lanes_kernel, levels, table),
        [
            shape((flat_rows, LANES), F32),
            shape((2 * SLAB, 2 * flat_rows - levels[1].span), BF16),
        ],
        [r, m_prev, m_next, *far, table_array],
        flops=1 << 26,
    )
    slabs = z_pair(slabs, "gz")

    fine = call(
        functools.partial(fine_kernel, zero),
        shape(charges.shape, F32),
        [wide, halo, lanes, band],
        scratch=[
            pltpu.VMEM((*zero.inp, 4 * LANES), BF16),
            pltpu.VMEM((4, zero.out[1], zero.inp[0], LANES), BF16),
        ],
        flops=1 << 32,
    )
    return call(
        functools.partial(coarse_kernel, levels, table),
        shape(charges.shape, BF16),
        [flat, slabs, lanes, band, table_array, fine],
        scratch=[pltpu.VMEM((*lv.inp, 4 * LANES), BF16) for lv in coarse]
        + [pltpu.VMEM((4, lv.out[1], lv.inp[0], LANES), BF16) for lv in coarse]
        + [pltpu.VMEM((*lv.out, LANES), F32) for lv in coarse],
        flops=1 << 31,
    )


def solution(mesh):
    return jax.shard_map(
        per_device,
        mesh=mesh,
        in_specs=(P("gx", "gy", "gz"), P()),
        out_specs=P("gx", "gy", "gz"),
        check_vma=False,
    )
```

```python
import functools

import jax
import jax.numpy as jnp
import numpy as np
from jax import lax
from jax.experimental import pallas as pl
from jax.experimental.pallas import tpu as pltpu
from jax.sharding import PartitionSpec as P

F32, BF16 = jnp.float32, jnp.bfloat16
REACH = 8
LANES = 128
TILE = 16
SLAB = 16
LOW, HIGH = (0, 1, 2, 2), (0, 2, 3, 3)
STENCIL = ((0, 1.0), (-1, 9 / 16), (1, 9 / 16), (-3, -1 / 16), (3, -1 / 16))


def up_to(value, step):
    return -(-value // step) * step


class Level:
    def __init__(self, index, block):
        self.index = index
        self.n = tuple(size >> index for size in block)
        self.low, self.high = LOW[index], HIGH[index]
        self.win = tuple(size + self.low + self.high for size in self.n)
        self.full = tuple(size + 2 * REACH for size in self.win)
        self.out = tuple(up_to(size, TILE) for size in self.win[:2])
        self.inp = tuple(size + TILE for size in self.out)
        self.rows = up_to(self.win[1], 8)
        self.lane = 0
        self.start = 0
        self.span = up_to(self.full[0] * self.inp[1], LANES)


def levels_of(block):
    levels = [Level(index, block) for index in range(4)]
    lane, start = 0, 0
    for level in levels[1:]:
        level.lane, level.start = lane, start
        lane += level.win[2]
        start += level.span
    assert lane <= LANES and block[2] == LANES
    assert all(level.n[d] % 8 == 0 for level in levels for d in range(3))
    return levels


def own_lane(level, z):
    return (level.lane + z + level.low + REACH) % LANES


def restrict_rows(coarse, fine):
    fine_rows = fine.n[1] if fine.index == 0 else fine.rows
    matrix = np.zeros((coarse.rows, 2, fine_rows))
    for row in range(coarse.win[1]):
        for offset, weight in STENCIL:
            col = 2 * (row - coarse.low) + offset + fine.low
            if 0 <= col < fine.win[1]:
                matrix[row, :, col] = weight
    return matrix.reshape(coarse.rows, 2 * fine_rows)


def restrict_lanes(coarse, fine):
    matrix = np.zeros((2, LANES, LANES))
    for z in range(-coarse.low, coarse.n[2] + coarse.high):
        for offset, weight in STENCIL:
            at = 2 * z + offset
            if -fine.low <= at < fine.n[2] + fine.high:
                lane = at if fine.index == 0 else own_lane(fine, at)
                matrix[:, lane, own_lane(coarse, z)] = weight
    return matrix.reshape(2 * LANES, LANES)


def prolong_weights(fine_at):
    half = fine_at // 2
    if fine_at % 2 == 0:
        return ((half, 1.0),)
    return ((half, 9 / 16), (half + 1, 9 / 16), (half - 1, -1 / 16), (half + 2, -1 / 16))


def prolong_matrix(fine_count, fine_win, fine_low, coarse_count, coarse_low):
    matrix = np.zeros((fine_count, coarse_count))
    for row in range(fine_win):
        for at, weight in prolong_weights(row - fine_low):
            if 0 <= at + coarse_low < coarse_count:
                matrix[row, at + coarse_low] = weight
    return matrix


def prolong_rows(fine, coarse):
    matrix = prolong_matrix(fine.out[1], fine.win[1], fine.low, coarse.out[1], coarse.low)
    return np.concatenate([matrix, matrix], 1)


def prolong_lanes(fine, coarse):
    matrix = prolong_matrix(LANES, fine.win[2], fine.low, LANES, coarse.low).T
    return np.concatenate([matrix, matrix], 0)


def send_lanes(level):
    up, down = np.zeros((SLAB, LANES)), np.zeros((SLAB, LANES))
    for j in range(SLAB):
        s = level.n[2] - REACH + j
        if s < level.win[2]:
            up[j, own_lane(level, s - level.low)] = 1
        if j < level.low + level.high + REACH:
            down[j, own_lane(level, j - level.low)] = 1
    return np.concatenate([up, down], 0)


def place_lanes(level):
    from_prev, from_next = np.zeros((SLAB, LANES)), np.zeros((SLAB, LANES))
    for j in range(SLAB):
        if level.n[2] - REACH + j < level.win[2]:
            from_prev[j, (level.lane + j) % LANES] = 1
        at = j + REACH + level.n[2]
        if at < level.full[2]:
            from_next[j, (level.lane + at) % LANES] = 1
    return np.concatenate([from_prev, from_next] * (1 if level.index == 1 else 2), 0)


def dot(a, b, dims=((1,), (0,))):
    return lax.dot_general(a, b, (dims, ((), ())), preferred_element_type=F32)


def split_rows(x):
    high = x.astype(BF16).astype(F32)
    return jnp.concatenate([high, x - high], 0).astype(BF16)


def split_lanes(x):
    high = x.astype(BF16).astype(F32)
    return jnp.concatenate([high, x - high], 1).astype(BF16)


class Table:
    def __init__(self):
        self.parts, self.places, self.count = [], {}, 0

    def add(self, key, matrix):
        rows, cols = matrix.shape
        padded = np.zeros((up_to(rows, TILE), LANES), np.float32)
        padded[:rows, :cols] = matrix
        self.places[key] = (self.count, rows, cols)
        self.parts.append(padded)
        self.count += padded.shape[0]

    def array(self):
        return jnp.asarray(np.concatenate(self.parts, 0), BF16)

    def get(self, ref, *key):
        start, rows, cols = self.places[key]
        return ref[start : start + rows, :cols]


def pad_rows(x, rows):
    if x.shape[0] == rows:
        return x
    return jnp.concatenate([x, jnp.zeros((rows - x.shape[0], x.shape[1]), x.dtype)], 0)


def total(terms):
    return functools.reduce(lambda a, b: a + b, terms)


def bands_kernel(levels, taps_ref, band_ref, lanes_ref):
    row = lax.broadcasted_iota(jnp.int32, (8 * TILE, 16 * TILE), 0)
    col = lax.broadcasted_iota(jnp.int32, (8 * TILE, 16 * TILE), 1)
    offset = jnp.where(row % 8 == col // 32, col % 32 - row // 8, -1)

    @pl.loop(0, 16)
    def _(which):
        matrix = jnp.zeros(offset.shape, F32)
        for tap in range(17):
            matrix = jnp.where(offset == tap, taps_ref[which, tap], matrix)
        band_ref[which] = matrix.astype(BF16)

    for level in levels:
        first, count = lane_rows(level)
        k = lax.broadcasted_iota(jnp.int32, (count, LANES), 0)
        z_out = lax.broadcasted_iota(jnp.int32, (count, LANES), 1)
        if level.index == 0:
            n = level.n[2]
            z_in = jnp.where(k < n, k + REACH, jnp.where(k < n + REACH, k - n, k))
            valid = k < n + 2 * REACH
        else:
            z_in = (k + (LANES - level.lane)) % LANES
            valid = (z_in < level.full[2]) & (z_out < level.win[2])
        offset_z = jnp.where(valid, z_in - z_out, -1)
        for term in range(4):
            matrix = jnp.zeros(offset_z.shape, F32)
            for tap in range(17):
                matrix = jnp.where(offset_z == tap, taps_ref[4 * level.index + term, tap], matrix)
            lanes_ref[first : first + count, term_lanes(term)] = matrix.astype(BF16)


def lane_rows(level):
    return (0, 2 * LANES) if level.index == 0 else ((level.index + 1) * LANES, LANES)


def term_lanes(term):
    return slice(term * LANES, (term + 1) * LANES)


def plane_at(levels, level, which, rows):
    first = 0
    for other in levels[1:]:
        sizes = (other.win[0], other.rows) if rows == "own" else (other.full[0], other.rows)
        if other is level:
            return slice(first + which * sizes[1], first + (which + 1) * sizes[1])
        first += sizes[0] * sizes[1]
    return first


def halves_of(x):
    high = x.astype(BF16).astype(F32)
    return high, x - high


def restrict_kernel(levels, table, charges_ref, table_ref, q_ref, up_ref, down_ref, far_ref):
    for level, fine in zip(levels[1:], levels[:3]):
        for at in range(level.win[0]):
            terms = {}
            for offset, weight in STENCIL:
                plane = 2 * (at - level.low) + offset + fine.low
                if 0 <= plane < fine.win[0]:
                    if fine.index == 0:
                        value = charges_ref[plane].astype(F32)
                    else:
                        value = q_ref[plane_at(levels, fine, plane, "own")]
                    terms.setdefault(weight, []).append(value)
            value = total([total(group) * weight for weight, group in terms.items()])
            value = dot(table.get(table_ref, "rows", level.index), split_rows(value))
            value = dot(split_lanes(value), table.get(table_ref, "lanes", level.index))
            q_ref[plane_at(levels, level, at, "own")] = value
    rows, rest_rows = levels[1].rows, levels[2].rows
    for j in range(up_ref.shape[0]):
        for slab_ref, bases in ((up_ref, [lv.n[0] - REACH for lv in levels[1:]]), (down_ref, [0] * 3)):
            highs, rests = [], [jnp.zeros((rest_rows, LANES), F32)]
            for level, base in zip(levels[1:], bases):
                if base + j < level.win[0]:
                    high, rest = halves_of(q_ref[plane_at(levels, level, base + j, "own")])
                    highs.append(pad_rows(high, rows))
                    if level.index > 1:
                        rests.append(pad_rows(rest, rest_rows))
            slab_ref[j] = jnp.concatenate([total(highs), total(rests)], 0).astype(BF16)
    last = levels[3]
    pack_far(
        far_ref,
        [q_ref[plane_at(levels, last, at, "own")] for at in range(last.win[0])],
    )


def pack_far(far_ref, planes):
    for group in range(far_ref.shape[0]):
        members = planes[4 * group : 4 * group + 4]
        far_ref[group] = total(
            [pltpu.roll(x, 32 * k, 1) if k else x for k, x in enumerate(members)]
        )


def unpack_far(far_ref, at):
    x = far_ref[at // 4]
    return pltpu.roll(x, LANES - 32 * (at % 4), 1) if at % 4 else x


def lane_masks(levels):
    lane = lax.broadcasted_iota(jnp.int32, (8, LANES), 1)
    masks = []
    for level in levels[1:]:
        at = (lane + (2 * LANES - level.lane - REACH)) % LANES
        masks.append((at < level.win[2])[:1])
    return masks


def rows_kernel(levels, q_ref, prev_ref, next_ref, far_prev_ref, *refs):
    far_next_ref = far_prev_ref if len(refs) == 4 else refs[0]
    x_ref, up_ref, down_ref, far_ref = refs[-4:]
    count, high_rows = prev_ref.shape[0], levels[1].rows
    masks = lane_masks(levels)
    coarsest = []

    def received(ref, at, level):
        slab = ref[at].astype(F32)
        high = slab[: level.rows]
        return high if level.index == 1 else high + slab[high_rows : high_rows + level.rows]

    rest_count = levels[2].full[0]
    for at in range(levels[1].full[0]):
        ups, downs = [], []
        for level, mask in zip(levels[1:], masks):
            if at >= level.full[0]:
                continue
            n = level.n[0]
            terms = []
            if 0 <= at - REACH < level.win[0]:
                terms.append(q_ref[plane_at(levels, level, at - REACH, "own")])
            if at < count and at - REACH + n < level.win[0]:
                terms.append(received(prev_ref, at, level))
            if 0 <= at - REACH - n < count:
                terms.append(received(next_ref, at - REACH - n, level))
            if level.index == 3:
                if at - REACH + 2 * n < level.win[0]:
                    terms.append(unpack_far(far_prev_ref, at - REACH + 2 * n))
                if at - REACH - 2 * n >= 0:
                    terms.append(unpack_far(far_next_ref, at - REACH - 2 * n))
            value = jnp.where(mask, total(terms), 0.0)
            x_ref[plane_at(levels, level, at, "full")] = value
            first = level.n[1] - REACH
            ups.append((level.index, halves_of(value[first : first + SLAB])))
            downs.append((level.index, halves_of(value[:SLAB])))
            if level.index == 3:
                coarsest.append(value)
        for slab_ref, parts in ((up_ref, ups), (down_ref, downs)):
            slab_ref[at] = total([x for _, (x, _) in parts]).astype(BF16)
            rests = [x for index, (_, x) in parts if index > 1]
            if rests:
                slab_ref[levels[1].full[0] + at] = total(rests).astype(BF16)
    pack_far(far_ref, coarsest)


def lanes_kernel(levels, table, x_ref, prev_ref, next_ref, far_prev_ref, *refs):
    far_next_ref = far_prev_ref if len(refs) == 3 else refs[0]
    table_ref, flat_ref, slab_ref = refs[-3:]

    def received(ref, at, level):
        high = ref[at].astype(F32)
        return high if level.index == 1 else high + ref[levels[1].full[0] + at].astype(F32)

    for level, mask in zip(levels[1:], lane_masks(levels)):
        blocks, step = level.inp[1] // 8, level.n[1] // 8
        for at in range(level.full[0]):
            own = x_ref[plane_at(levels, level, at, "full")]
            slabs = [received(prev_ref, at, level), received(next_ref, at, level)]
            if level.index == 3:
                slabs += [unpack_far(far_prev_ref, at), unpack_far(far_next_ref, at)]
            parts = []
            for block in range(blocks):
                terms = []
                if 0 <= block - 1 < level.rows // 8:
                    terms.append(own[8 * block - 8 : 8 * block])
                places = [block, block - 1 - step, block - 1 + 2 * step, block - 1 - 2 * step]
                for slab, place in zip(slabs, places):
                    if 0 <= place < SLAB // 8:
                        terms.append(slab[8 * place : 8 * place + 8])
                parts.append(total(terms) if terms else jnp.zeros((8, LANES), F32))
            value = jnp.where(mask, jnp.concatenate(parts, 0), 0.0)
            first = level.start + at * level.inp[1]
            flat_ref[first : first + level.inp[1]] = value
        used = level.start + level.full[0] * level.inp[1]
        last = level.start + level.span
        if used < last:
            flat_ref[used:last] = jnp.zeros((last - used, LANES), F32)
    shift = levels[-1].start + levels[-1].span - levels[2].start
    for level in levels[1:]:
        send = table.get(table_ref, "send", level.index)
        for first in range(level.start, level.start + level.span, 512):
            stop = min(first + 512, level.start + level.span)
            high, rest = halves_of(flat_ref[first:stop])
            slab_ref[:, first:stop] = dot(send, high.astype(BF16), ((1,), (1,))).astype(BF16)
            if level.index > 1:
                slab_ref[:, first + shift : stop + shift] = dot(
                    send, rest.astype(BF16), ((1,), (1,))
                ).astype(BF16)


def halo_kernel(wide_ref, out_ref):
    planes, rows, count = wide_ref.shape
    row = lax.broadcasted_iota(jnp.int32, (2 * REACH, count), 0)
    lane = lax.broadcasted_iota(jnp.int32, (2 * REACH, count), 1)
    send = jnp.where(lane == (row + (count - REACH)) % count, 1.0, 0.0).astype(BF16)
    step = 8
    for first in range(0, planes, step):
        chunk = wide_ref[first : first + step].reshape(step * rows, LANES)
        out_ref[:, first * rows : (first + step) * rows] = dot(send, chunk, ((1,), (1,))).astype(BF16)


def two_passes(level, band, first_ref, second_ref, put):
    def parts_of(result):
        parts = [result[:, :LANES], result[:, LANES:]]
        return jnp.concatenate([x.reshape(TILE, 8, LANES) for x in parts], 1)

    def along_y(pair):
        for block in range(level.out[1] // TILE):
            for term in range(4):
                halves = [
                    first_ref[
                        pl.ds(pair * 16 + 8 * half, 8),
                        TILE * block : TILE * block + 32,
                        term_lanes(term),
                    ].reshape(256, LANES)
                    for half in range(2)
                ]
                result = dot(band(term), jnp.concatenate(halves, 1))
                second_ref[
                    term, TILE * block : TILE * (block + 1), pl.ds(pl.multiple_of(pair * 16, 16), 16)
                ] = parts_of(result).astype(BF16)

    def along_x(pair):
        for block in range(level.out[0] // TILE):
            result = None
            for term in range(4):
                halves = [
                    second_ref[
                        term, pl.ds(pair * 16 + 8 * half, 8), TILE * block : TILE * block + 32
                    ].reshape(256, LANES)
                    for half in range(2)
                ]
                part = dot(band(term), jnp.concatenate(halves, 1))
                result = part if result is None else result + part
            put(block, pair, parts_of(result))

    pl.loop(0, level.inp[0] // 16)(along_y)
    pl.loop(0, level.out[1] // 16)(along_x)


def fine_kernel(level, wide_ref, halo_ref, lanes_ref, band_ref, out_ref, first_ref, second_ref):
    rows, step = level.inp[1], 8
    row = lax.broadcasted_iota(jnp.int32, (2 * REACH, LANES), 0)
    lane = lax.broadcasted_iota(jnp.int32, (2 * REACH, LANES), 1)
    place = jnp.where(lane == row, 1.0, 0.0).astype(BF16)

    @pl.loop(0, level.inp[0] // step)
    def _(chunk):
        where = pl.ds(pl.multiple_of(chunk * step * rows, LANES), step * rows)
        sides = dot(halo_ref[:, where], place, ((0,), (0,))).astype(BF16)
        here = wide_ref[pl.ds(chunk * step, step)].reshape(step * rows, LANES)
        result = dot(jnp.concatenate([here, sides], 1), lanes_ref[: 2 * LANES])
        first_ref[pl.ds(chunk * step, step)] = result.astype(BF16).reshape(step, rows, 4 * LANES)

    def put(block, pair, value):
        out_ref[TILE * block : TILE * (block + 1), pl.ds(pl.multiple_of(pair * 16, 16), 16)] = value

    two_passes(level, lambda term: band_ref[term], first_ref, second_ref, put)


def coarse_kernel(levels, table, flat_ref, slab_ref, lanes_ref, band_ref, table_ref, fine_ref, *refs):
    out_ref, first_refs, second_refs, sum_refs = refs[0], refs[1:4], refs[4:7], refs[7:10]
    shift = levels[-1].start + levels[-1].span - levels[2].start
    for level in reversed(levels[1:]):
        which = level.index - 1
        first_ref, sum_ref = first_refs[which], sum_refs[which]
        rows, step = level.inp[1], 4
        first_lane, _ = lane_rows(level)
        place = table.get(table_ref, "place", level.index)
        for plane in range(0, level.full[0], step):
            count = min(step, level.full[0] - plane)
            if (count * rows) % LANES:
                count += 1
            start, stop = level.start + plane * rows, level.start + (plane + count) * rows
            slab = slab_ref[:, start:stop]
            if level.index > 1:
                slab = jnp.concatenate([slab, slab_ref[:, start + shift : stop + shift]], 0)
            value = flat_ref[start:stop] + dot(slab, place, ((0,), (0,)))
            result = dot(value.astype(BF16), lanes_ref[first_lane : first_lane + LANES])
            first_ref[plane : plane + count] = result.astype(BF16).reshape(count, rows, 4 * LANES)
        rest = level.inp[0] - plane - count
        if rest > 0:
            first_ref[plane + count :] = jnp.zeros((rest, rows, 4 * LANES), BF16)

        def put(block, pair, value, sum_ref=sum_ref):
            sum_ref[TILE * block : TILE * (block + 1), pl.ds(pl.multiple_of(pair * 16, 16), 16)] = value

        base = 4 * level.index
        two_passes(level, lambda term, base=base: band_ref[base + term], first_ref, second_refs[which], put)

    def stretch(fine, coarse, source):
        planes, rows, _ = source.shape
        for first in range(0, coarse.win[0], 4):
            count = min(4, planes - first)
            value = split_lanes(source[first : first + count].reshape(count * rows, LANES))
            value = dot(value, table.get(table_ref, "zed", fine.index))
            source[first : first + count] = value.reshape(count, rows, LANES)

    def prolong(fine, coarse, halves, source, emit):
        planes = []
        for half in halves:
            at = half + coarse.low
            between = (9.0 * (source[at] + source[at + 1]) - (source[at - 1] + source[at + 2])) / 16.0
            planes += [split_rows(source[at]), split_rows(between)]
        both = dot(table.get(table_ref, "tall", fine.index), jnp.concatenate(planes, 1))
        for k, half in enumerate(halves):
            emit(2 * half, both[:, 2 * k * LANES : (2 * k + 1) * LANES])
            emit(2 * half + 1, both[:, (2 * k + 1) * LANES : (2 * k + 2) * LANES])

    for fine, coarse in ((levels[2], levels[3]), (levels[1], levels[2])):
        sum_ref = sum_refs[fine.index - 1]
        source = sum_refs[coarse.index - 1]
        stretch(fine, coarse, source)

        def emit(at, value, fine=fine, sum_ref=sum_ref):
            plane = at + fine.low
            if 0 <= plane < fine.win[0]:
                sum_ref[plane] = sum_ref[plane] + value

        for half in range(-1, (fine.n[0] + fine.high + 1) // 2):
            prolong(fine, coarse, [half], source, emit)

    stretch(levels[0], levels[1], sum_refs[0])

    @pl.loop(0, levels[0].n[0] // 8)
    def _(group):
        def emit(at, value):
            out_ref[at] = (fine_ref[at] + value).astype(BF16)

        prolong(levels[0], levels[1], [4 * group + k for k in range(4)], sum_refs[0], emit)


def make_table(levels):
    table = Table()
    for level, fine in zip(levels[1:], levels[:3]):
        table.add(("rows", level.index), restrict_rows(level, fine))
        table.add(("lanes", level.index), restrict_lanes(level, fine))
        table.add(("send", level.index), send_lanes(level))
        table.add(("place", level.index), place_lanes(level))
        table.add(("tall", fine.index), prolong_rows(fine, level))
        table.add(("zed", fine.index), prolong_lanes(fine, level))
    return table


def call(kernel, out_shape, args, scratch=(), smem=(), flops=0, limit=12):
    specs = [
        pl.BlockSpec(memory_space=pltpu.SMEM if i in smem else pltpu.VMEM) for i in range(len(args))
    ]
    single = not isinstance(out_shape, (list, tuple))
    outs = [out_shape] if single else list(out_shape)
    out_specs = [pl.BlockSpec(memory_space=pltpu.VMEM) for _ in outs]
    return pl.pallas_call(
        kernel,
        out_shape=out_shape,
        in_specs=specs,
        out_specs=out_specs[0] if single else out_specs,
        scratch_shapes=list(scratch),
        compiler_params=pltpu.CompilerParams(vmem_limit_bytes=limit << 20),
        cost_estimate=pl.CostEstimate(flops=flops, bytes_accessed=1 << 20, transcendentals=0),
    )(*args)


def shape(sizes, dtype):
    return jax.ShapeDtypeStruct(tuple(sizes), dtype)


def shifted(value, axis, by):
    count = lax.axis_size(axis)
    return lax.ppermute(value, axis, [(i, (i + by) % count) for i in range(count)])


def far_pair(value, axis):
    after = shifted(value, axis, 2)
    return [after] if lax.axis_size(axis) == 4 else [after, shifted(value, axis, -2)]


def z_pair(value, axis):
    half = value.shape[0] // 2
    if lax.axis_size(axis) == 2:
        return shifted(value, axis, 1)
    return jnp.concatenate([shifted(value[:half], axis, 1), shifted(value[half:], axis, -1)], 0)


def per_device(charges, taps):
    levels = levels_of(charges.shape)
    table = make_table(levels)
    table_array = table.array()
    zero, coarse = levels[0], levels[1:]
    reach = REACH

    x_prev = shifted(charges[-reach:], "gx", 1)
    x_next = shifted(charges[:reach], "gx", -1)

    slab_planes = max(level.low + level.high + reach for level in coarse)
    slab_rows = levels[1].rows + levels[2].rows
    q, l_up, l_down, l_far = call(
        functools.partial(restrict_kernel, levels, table),
        [shape((sum(lv.win[0] * lv.rows for lv in coarse), LANES), F32)]
        + [shape((slab_planes, slab_rows, LANES), BF16)] * 2
        + [shape((up_to(levels[3].win[0], 4) // 4, SLAB, LANES), F32)],
        [charges, table_array],
        flops=1 << 27,
    )
    band, lanes = call(
        functools.partial(bands_kernel, levels),
        [shape((16, 8 * TILE, 16 * TILE), BF16), shape((5 * LANES, 4 * LANES), BF16)],
        [taps.reshape(16, 17)],
        smem=(0,),
        flops=1 << 26,
    )

    l_prev = shifted(l_up, "gx", 1)
    l_next = shifted(l_down, "gx", -1)
    far = far_pair(l_far, "gx")

    pieces = (x_prev, charges, x_next)
    y_prev = shifted(jnp.concatenate([x[:, -reach:] for x in pieces], 0), "gy", 1)
    y_next = shifted(jnp.concatenate([x[:, :reach] for x in pieces], 0), "gy", -1)

    r, m_up, m_down, m_far = call(
        functools.partial(rows_kernel, levels),
        [shape((sum(lv.full[0] * lv.rows for lv in coarse), LANES), F32)]
        + [shape((levels[1].full[0] + levels[2].full[0], SLAB, LANES), BF16)] * 2
        + [shape((up_to(levels[3].full[0], 4) // 4, SLAB, LANES), F32)],
        [q, l_prev, l_next, *far],
        flops=1 << 25,
    )
    m_prev = shifted(m_up, "gy", 1)
    m_next = shifted(m_down, "gy", -1)
    far = far_pair(m_far, "gy")

    wide = jnp.concatenate([y_prev, jnp.concatenate(pieces, 0), y_next], 1)
    sides = call(
        halo_kernel,
        shape((2 * reach, wide.shape[0] * wide.shape[1]), BF16),
        [wide],
        flops=1 << 26,
    )
    halo = z_pair(sides, "gz")

    flat_rows = sum(level.span for level in coarse)
    flat, slabs = call(
        functools.partial(lanes_kernel, levels, table),
        [
            shape((flat_rows, LANES), F32),
            shape((2 * SLAB, 2 * flat_rows - levels[1].span), BF16),
        ],
        [r, m_prev, m_next, *far, table_array],
        flops=1 << 26,
    )
    slabs = z_pair(slabs, "gz")

    fine = call(
        functools.partial(fine_kernel, zero),
        shape(charges.shape, F32),
        [wide, halo, lanes, band],
        scratch=[
            pltpu.VMEM((*zero.inp, 4 * LANES), BF16),
            pltpu.VMEM((4, zero.out[1], zero.inp[0], LANES), BF16),
        ],
        flops=1 << 32,
        limit=24,
    )
    return call(
        functools.partial(coarse_kernel, levels, table),
        shape(charges.shape, BF16),
        [flat, slabs, lanes, band, table_array, fine],
        scratch=[pltpu.VMEM((*lv.inp, 4 * LANES), BF16) for lv in coarse]
        + [pltpu.VMEM((4, lv.out[1], lv.inp[0], LANES), BF16) for lv in coarse]
        + [pltpu.VMEM((*lv.out, LANES), F32) for lv in coarse],
        flops=1 << 31,
        limit=30,
    )


def solution(mesh):
    return jax.shard_map(
        per_device,
        mesh=mesh,
        in_specs=(P("gx", "gy", "gz"), P()),
        out_specs=P("gx", "gy", "gz"),
        check_vma=False,
    )
```

```python
import functools

import jax
import jax.numpy as jnp
import numpy as np
from jax import lax
from jax.experimental import pallas as pl
from jax.experimental.pallas import tpu as pltpu
from jax.sharding import PartitionSpec as P


F32, BF16 = jnp.float32, jnp.bfloat16
REACH = 8
LANES = 128
TILE = 16
SLAB = 16
LOW, HIGH = (0, 1, 2, 2), (0, 2, 3, 3)
STENCIL = ((0, 1.0), (-1, 9 / 16), (1, 9 / 16), (-3, -1 / 16), (3, -1 / 16))


def up_to(value, step):
    return -(-value // step) * step


class Level:
    def __init__(self, index, block):
        self.index = index
        self.n = tuple(size >> index for size in block)
        self.low, self.high = LOW[index], HIGH[index]
        self.win = tuple(size + self.low + self.high for size in self.n)
        self.full = tuple(size + 2 * REACH for size in self.win)
        self.out = tuple(up_to(size, TILE) for size in self.win[:2])
        self.inp = tuple(size + TILE for size in self.out)
        self.rows = up_to(self.win[1], 8)
        self.lane = 0
        self.start = 0
        self.span = up_to(self.full[0] * self.inp[1], LANES)


def levels_of(block):
    levels = [Level(index, block) for index in range(4)]
    lane, start = 0, 0
    for level in levels[1:]:
        level.lane, level.start = lane, start
        lane += level.win[2]
        start += level.span
    assert lane <= LANES and block[2] == LANES
    assert all(level.n[d] % 8 == 0 for level in levels for d in range(3))
    return levels


def own_lane(level, z):
    return (level.lane + z + level.low + REACH) % LANES


def stencil_of(offset, valid):
    size = jnp.abs(offset)
    weight = jnp.where(size == 0, 1.0, jnp.where(size == 1, 9 / 16, jnp.where(size == 3, -1 / 16, 0.0)))
    return jnp.where(valid, weight, 0.0).astype(BF16)


def restrict_rows(coarse, fine):
    fine_rows = fine.n[1] if fine.index == 0 else fine.rows
    row = lax.broadcasted_iota(jnp.int32, (coarse.rows, 2 * fine_rows), 0)
    col = lax.broadcasted_iota(jnp.int32, (coarse.rows, 2 * fine_rows), 1)
    col = jnp.where(col >= fine_rows, col - fine_rows, col)
    valid = (row < coarse.win[1]) & (col < fine.win[1])
    return stencil_of(col - fine.low - 2 * (row - coarse.low), valid)


def restrict_lanes(coarse, fine):
    k = lax.broadcasted_iota(jnp.int32, (2 * LANES, LANES), 0) % LANES
    lane = lax.broadcasted_iota(jnp.int32, (2 * LANES, LANES), 1)

    def place(level, lanes):
        return lanes if level.index == 0 else (lanes + (2 * LANES - level.lane - REACH)) % LANES

    k, lane = place(fine, k), place(coarse, lane)
    valid = (k < fine.win[2]) & (lane < coarse.win[2])
    return stencil_of(k - fine.low - 2 * (lane - coarse.low), valid)


def prolong_weights(fine_at):
    half = fine_at // 2
    if fine_at % 2 == 0:
        return ((half, 1.0),)
    return ((half, 9 / 16), (half + 1, 9 / 16), (half - 1, -1 / 16), (half + 2, -1 / 16))


def prolong_matrix(fine_count, fine_win, fine_low, coarse_count, coarse_low):
    matrix = np.zeros((fine_count, coarse_count))
    for row in range(fine_win):
        for at, weight in prolong_weights(row - fine_low):
            if 0 <= at + coarse_low < coarse_count:
                matrix[row, at + coarse_low] = weight
    return matrix


def prolong_rows(fine, coarse):
    matrix = prolong_matrix(fine.out[1], fine.win[1], fine.low, coarse.out[1], coarse.low)
    return np.concatenate([matrix, matrix], 1)


def prolong_lanes(fine, coarse):
    matrix = prolong_matrix(LANES, fine.win[2], fine.low, LANES, coarse.low).T
    return np.concatenate([matrix, matrix], 0)


def send_lanes(level):
    up, down = np.zeros((SLAB, LANES)), np.zeros((SLAB, LANES))
    for j in range(SLAB):
        s = level.n[2] - REACH + j
        if s < level.win[2]:
            up[j, own_lane(level, s - level.low)] = 1
        if j < level.low + level.high + REACH:
            down[j, own_lane(level, j - level.low)] = 1
    return np.concatenate([up, down], 0)


def place_lanes(level):
    from_prev, from_next = np.zeros((SLAB, LANES)), np.zeros((SLAB, LANES))
    for j in range(SLAB):
        if level.n[2] - REACH + j < level.win[2]:
            from_prev[j, (level.lane + j) % LANES] = 1
        at = j + REACH + level.n[2]
        if at < level.full[2]:
            from_next[j, (level.lane + at) % LANES] = 1
    return np.concatenate([from_prev, from_next] * (1 if level.index == 1 else 2), 0)


def dot(a, b, dims=((1,), (0,))):
    return lax.dot_general(a, b, (dims, ((), ())), preferred_element_type=F32)


def split_rows(x):
    high = x.astype(BF16).astype(F32)
    return jnp.concatenate([high, x - high], 0).astype(BF16)


def split_lanes(x):
    high = x.astype(BF16).astype(F32)
    return jnp.concatenate([high, x - high], 1).astype(BF16)


class Table:
    def __init__(self):
        self.parts, self.places, self.count = [], {}, 0

    def add(self, key, matrix):
        rows, cols = matrix.shape
        padded = np.zeros((up_to(rows, TILE), LANES), np.float32)
        padded[:rows, :cols] = matrix
        self.places[key] = (self.count, rows, cols)
        self.parts.append(padded)
        self.count += padded.shape[0]

    def array(self):
        return jnp.asarray(np.concatenate(self.parts, 0), BF16)

    def get(self, ref, *key):
        start, rows, cols = self.places[key]
        return ref[start : start + rows, :cols]


def pad_rows(x, rows):
    if x.shape[0] == rows:
        return x
    return jnp.concatenate([x, jnp.zeros((rows - x.shape[0], x.shape[1]), x.dtype)], 0)


def total(terms):
    return functools.reduce(lambda a, b: a + b, terms)


def bands_kernel(levels, taps_ref, band_ref, lanes_ref):
    row = lax.broadcasted_iota(jnp.int32, (8 * TILE, 16 * TILE), 0)
    col = lax.broadcasted_iota(jnp.int32, (8 * TILE, 16 * TILE), 1)
    offset = jnp.where(row % 8 == col // 32, col % 32 - row // 8, -1)

    @pl.loop(0, 16)
    def _(which):
        matrix = jnp.zeros(offset.shape, F32)
        for tap in range(17):
            matrix = jnp.where(offset == tap, taps_ref[which, tap], matrix)
        band_ref[which] = matrix.astype(BF16)

    for level in levels:
        first, count = lane_rows(level)
        k = lax.broadcasted_iota(jnp.int32, (count, LANES), 0)
        z_out = lax.broadcasted_iota(jnp.int32, (count, LANES), 1)
        if level.index == 0:
            n = level.n[2]
            z_in = jnp.where(k < n, k + REACH, jnp.where(k < n + REACH, k - n, k))
            valid = k < n + 2 * REACH
        else:
            z_in = (k + (LANES - level.lane)) % LANES
            valid = (z_in < level.full[2]) & (z_out < level.win[2])
        offset_z = jnp.where(valid, z_in - z_out, -1)
        for term in range(4):
            matrix = jnp.zeros(offset_z.shape, F32)
            for tap in range(17):
                matrix = jnp.where(offset_z == tap, taps_ref[4 * level.index + term, tap], matrix)
            lanes_ref[first : first + count, term_lanes(term)] = matrix.astype(BF16)


def lane_rows(level):
    return (0, 2 * LANES) if level.index == 0 else ((level.index + 1) * LANES, LANES)


def term_lanes(term):
    return slice(term * LANES, (term + 1) * LANES)


def plane_at(levels, level, which, rows):
    first = 0
    for other in levels[1:]:
        sizes = (other.win[0], other.rows) if rows == "own" else (other.full[0], other.rows)
        if other is level:
            return slice(first + which * sizes[1], first + (which + 1) * sizes[1])
        first += sizes[0] * sizes[1]
    return first


def halves_of(x):
    high = x.astype(BF16).astype(F32)
    return high, x - high


def restrict_kernel(
    levels, charges_ref, q_ref, up_ref, down_ref, far_ref
):
    for level, fine in zip(levels[1:], levels[:3]):
        by_rows, by_lanes = restrict_rows(level, fine), restrict_lanes(level, fine)
        for at in range(level.win[0]):
            terms = {}
            for offset, weight in STENCIL:
                plane = 2 * (at - level.low) + offset + fine.low
                if 0 <= plane < fine.win[0]:
                    if fine.index == 0:
                        value = charges_ref[plane].astype(F32)
                    else:
                        value = q_ref[plane_at(levels, fine, plane, "own")]
                    terms.setdefault(weight, []).append(value)
            value = total([total(group) * weight for weight, group in terms.items()])
            value = dot(by_rows, split_rows(value))
            value = dot(split_lanes(value), by_lanes)
            q_ref[plane_at(levels, level, at, "own")] = value
    high_rows, rest_rows = levels[1].rows, levels[2].rows
    pitch = slab_pitch(levels)
    planes = slab_planes(levels)
    for j in range(planes):
        for slab_ref, bases in ((up_ref, [lv.n[0] - REACH for lv in levels[1:]]), (down_ref, [0] * 3)):
            highs, rests = [], [jnp.zeros((rest_rows, LANES), F32)]
            for level, base in zip(levels[1:], bases):
                if base + j < level.win[0]:
                    high, rest = halves_of(q_ref[plane_at(levels, level, base + j, "own")])
                    highs.append(pad_rows(high, high_rows))
                    if level.index > 1:
                        rests.append(pad_rows(rest, rest_rows))
            rest = jnp.concatenate([jnp.zeros((rest_rows, LANES), F32), total(rests)], 0)
            value = pad_rows(total(highs), pitch) + rest
            slab_ref[j * pitch : (j + 1) * pitch] = value.astype(BF16)
    last = levels[3]
    pack_far(
        levels,
        far_ref,
        [q_ref[plane_at(levels, last, at, "own")] for at in range(last.win[0])],
    )


def slab_planes(levels):
    return max(level.low + level.high + REACH for level in levels[1:])


def slab_pitch(levels):
    return up_to(max(levels[1].rows, 2 * levels[2].rows), TILE)


def rest_block(levels, plane):
    spare = levels[1].full[0] - levels[2].full[0]
    if plane < spare:
        return levels[2].full[0] + plane, 0
    return levels[1].full[0] + (plane - spare) // 2, LANES // 2 * ((plane - spare) % 2)


def slab_blocks(levels):
    return rest_block(levels, levels[2].full[0] - 1)[0] + 1


def turned(x, lanes):
    return pltpu.roll(x, lanes % LANES, 1) if lanes % LANES else x


def far_groups(levels, planes):
    return -(-planes // (LANES // levels[3].win[2]))


def pack_far(levels, far_ref, planes):
    width = levels[3].win[2]
    per = LANES // width
    for group in range(far_ref.shape[0]):
        members = planes[per * group : per * group + per]
        far_ref[group] = total([turned(x, width * k) for k, x in enumerate(members)])


def unpack_far(levels, far_ref, at):
    width = levels[3].win[2]
    per = LANES // width
    return turned(far_ref[at // per], LANES - width * (at % per))


def lane_masks(levels):
    lane = lax.broadcasted_iota(jnp.int32, (8, LANES), 1)
    masks = []
    for level in levels[1:]:
        at = (lane + (2 * LANES - level.lane - REACH)) % LANES
        masks.append((at < level.win[2])[:1])
    return masks


def rows_kernel(levels, q_ref, prev_ref, next_ref, far_prev_ref, *refs):
    far_next_ref = far_prev_ref if len(refs) == 4 else refs[0]
    x_ref, up_ref, down_ref, far_ref = refs[-4:]
    count, pitch, rest_rows = slab_planes(levels), slab_pitch(levels), levels[2].rows
    masks = lane_masks(levels)
    coarsest = []

    def received(ref, at, level):
        slab = ref[at * pitch : (at + 1) * pitch].astype(F32)
        high = slab[: level.rows]
        return high if level.index == 1 else high + slab[rest_rows : rest_rows + level.rows]

    blocks = {True: {}, False: {}}
    for at in range(levels[1].full[0]):
        for level, mask in zip(levels[1:], masks):
            if at >= level.full[0]:
                continue
            n = level.n[0]
            terms = []
            if 0 <= at - REACH < level.win[0]:
                terms.append(q_ref[plane_at(levels, level, at - REACH, "own")])
            if at < count and at - REACH + n < level.win[0]:
                terms.append(received(prev_ref, at, level))
            if 0 <= at - REACH - n < count:
                terms.append(received(next_ref, at - REACH - n, level))
            if level.index == 3:
                if at - REACH + 2 * n < level.win[0]:
                    terms.append(unpack_far(levels, far_prev_ref, at - REACH + 2 * n))
                if at - REACH - 2 * n >= 0:
                    terms.append(unpack_far(levels, far_next_ref, at - REACH - 2 * n))
            value = jnp.where(mask, total(terms), 0.0)
            x_ref[plane_at(levels, level, at, "full")] = value
            first = level.n[1] - REACH
            for is_up, rows in ((True, value[first : first + SLAB]), (False, value[:SLAB])):
                high, rest = halves_of(rows)
                blocks[is_up].setdefault(at, []).append(high)
                if level.index > 1:
                    block, lanes = rest_block(levels, at)
                    blocks[is_up].setdefault(block, []).append(turned(rest, lanes))
            if level.index == 3:
                coarsest.append(value)
    for is_up, slab_ref in ((True, up_ref), (False, down_ref)):
        for block, parts in blocks[is_up].items():
            slab_ref[block * SLAB : (block + 1) * SLAB] = total(parts).astype(BF16)
    pack_far(levels, far_ref, coarsest)


def lanes_kernel(levels, table, x_ref, prev_ref, next_ref, far_prev_ref, *refs):
    far_next_ref = far_prev_ref if len(refs) == 3 else refs[0]
    table_ref, flat_ref, slab_ref = refs[-3:]

    def block_of(ref, block):
        return ref[block * SLAB : (block + 1) * SLAB].astype(F32)

    def received(ref, at, level):
        high = block_of(ref, at)
        if level.index == 1:
            return high
        block, lanes = rest_block(levels, at)
        return high + turned(block_of(ref, block), LANES - lanes)

    for level, mask in zip(levels[1:], lane_masks(levels)):
        blocks, step = level.inp[1] // 8, level.n[1] // 8
        for at in range(level.full[0]):
            own = x_ref[plane_at(levels, level, at, "full")]
            slabs = [received(prev_ref, at, level), received(next_ref, at, level)]
            if level.index == 3:
                slabs += [unpack_far(levels, ref, at) for ref in (far_prev_ref, far_next_ref)]
            parts = []
            for block in range(blocks):
                terms = []
                if 0 <= block - 1 < level.rows // 8:
                    terms.append(own[8 * block - 8 : 8 * block])
                places = [block, block - 1 - step, block - 1 + 2 * step, block - 1 - 2 * step]
                for slab, place in zip(slabs, places):
                    if 0 <= place < SLAB // 8:
                        terms.append(slab[8 * place : 8 * place + 8])
                parts.append(total(terms) if terms else jnp.zeros((8, LANES), F32))
            value = jnp.where(mask, jnp.concatenate(parts, 0), 0.0)
            first = level.start + at * level.inp[1]
            flat_ref[first : first + level.inp[1]] = value
        used = level.start + level.full[0] * level.inp[1]
        last = level.start + level.span
        if used < last:
            flat_ref[used:last] = jnp.zeros((last - used, LANES), F32)
    shift = levels[-1].start + levels[-1].span - levels[2].start
    for level in levels[1:]:
        send = table.get(table_ref, "send", level.index)
        for first in range(level.start, level.start + level.span, 512):
            stop = min(first + 512, level.start + level.span)
            high, rest = halves_of(flat_ref[first:stop])
            slab_ref[:, first:stop] = dot(send, high.astype(BF16), ((1,), (1,))).astype(BF16)
            if level.index > 1:
                slab_ref[:, first + shift : stop + shift] = dot(
                    send, rest.astype(BF16), ((1,), (1,))
                ).astype(BF16)


def halo_kernel(wide_ref, out_ref):
    planes, rows, count = wide_ref.shape
    row = lax.broadcasted_iota(jnp.int32, (2 * REACH, count), 0)
    lane = lax.broadcasted_iota(jnp.int32, (2 * REACH, count), 1)
    send = jnp.where(lane == (row + (count - REACH)) % count, 1.0, 0.0).astype(BF16)
    step = 8
    for first in range(0, planes, step):
        chunk = wide_ref[first : first + step].reshape(step * rows, LANES)
        out_ref[:, first * rows : (first + step) * rows] = dot(send, chunk, ((1,), (1,))).astype(BF16)


def two_passes(level, band, first_ref, second_ref, put):
    def parts_of(result):
        parts = [result[:, :LANES], result[:, LANES:]]
        return jnp.concatenate([x.reshape(TILE, 8, LANES) for x in parts], 1)

    def along_y(pair):
        for block in range(level.out[1] // TILE):
            for term in range(4):
                halves = [
                    first_ref[
                        pl.ds(pair * 16 + 8 * half, 8),
                        TILE * block : TILE * block + 32,
                        term_lanes(term),
                    ].reshape(256, LANES)
                    for half in range(2)
                ]
                result = dot(band(term), jnp.concatenate(halves, 1))
                second_ref[
                    term, TILE * block : TILE * (block + 1), pl.ds(pl.multiple_of(pair * 16, 16), 16)
                ] = parts_of(result).astype(BF16)

    def along_x(pair):
        for block in range(level.out[0] // TILE):
            result = None
            for term in range(4):
                halves = [
                    second_ref[
                        term, pl.ds(pair * 16 + 8 * half, 8), TILE * block : TILE * block + 32
                    ].reshape(256, LANES)
                    for half in range(2)
                ]
                part = dot(band(term), jnp.concatenate(halves, 1))
                result = part if result is None else result + part
            put(block, pair, parts_of(result))

    pl.loop(0, level.inp[0] // 16)(along_y)
    pl.loop(0, level.out[1] // 16)(along_x)


def fine_kernel(level, wide_ref, halo_ref, lanes_ref, band_ref, out_ref, first_ref, second_ref):
    rows, step = level.inp[1], 8
    row = lax.broadcasted_iota(jnp.int32, (2 * REACH, LANES), 0)
    lane = lax.broadcasted_iota(jnp.int32, (2 * REACH, LANES), 1)
    place = jnp.where(lane == row, 1.0, 0.0).astype(BF16)

    @pl.loop(0, level.inp[0] // step)
    def _(chunk):
        where = pl.ds(pl.multiple_of(chunk * step * rows, LANES), step * rows)
        sides = dot(halo_ref[:, where], place, ((0,), (0,))).astype(BF16)
        here = wide_ref[pl.ds(chunk * step, step)].reshape(step * rows, LANES)
        result = dot(jnp.concatenate([here, sides], 1), lanes_ref[: 2 * LANES])
        first_ref[pl.ds(chunk * step, step)] = result.astype(BF16).reshape(step, rows, 4 * LANES)

    def put(block, pair, value):
        out_ref[TILE * block : TILE * (block + 1), pl.ds(pl.multiple_of(pair * 16, 16), 16)] = value

    two_passes(level, lambda term: band_ref[term], first_ref, second_ref, put)


def coarse_kernel(levels, table, flat_ref, slab_ref, lanes_ref, band_ref, table_ref, fine_ref, *refs):
    out_ref, first_refs, second_refs, sum_refs = refs[0], refs[1:4], refs[4:7], refs[7:10]
    shift = levels[-1].start + levels[-1].span - levels[2].start
    for level in reversed(levels[1:]):
        which = level.index - 1
        first_ref, sum_ref = first_refs[which], sum_refs[which]
        rows, step = level.inp[1], 4
        first_lane, _ = lane_rows(level)
        place = table.get(table_ref, "place", level.index)
        for plane in range(0, level.full[0], step):
            count = min(step, level.full[0] - plane)
            if (count * rows) % LANES:
                count += 1
            start, stop = level.start + plane * rows, level.start + (plane + count) * rows
            slab = slab_ref[:, start:stop]
            if level.index > 1:
                slab = jnp.concatenate([slab, slab_ref[:, start + shift : stop + shift]], 0)
            value = flat_ref[start:stop] + dot(slab, place, ((0,), (0,)))
            result = dot(value.astype(BF16), lanes_ref[first_lane : first_lane + LANES])
            first_ref[plane : plane + count] = result.astype(BF16).reshape(count, rows, 4 * LANES)
        rest = level.inp[0] - plane - count
        if rest > 0:
            first_ref[plane + count :] = jnp.zeros((rest, rows, 4 * LANES), BF16)

        def put(block, pair, value, sum_ref=sum_ref):
            sum_ref[TILE * block : TILE * (block + 1), pl.ds(pl.multiple_of(pair * 16, 16), 16)] = value

        base = 4 * level.index
        two_passes(level, lambda term, base=base: band_ref[base + term], first_ref, second_refs[which], put)

    def stretch(fine, coarse, source):
        planes, rows, _ = source.shape
        for first in range(0, coarse.win[0], 4):
            count = min(4, planes - first)
            value = split_lanes(source[first : first + count].reshape(count * rows, LANES))
            value = dot(value, table.get(table_ref, "zed", fine.index))
            source[first : first + count] = value.reshape(count, rows, LANES)

    def prolong(fine, coarse, halves, source, emit):
        planes = []
        for half in halves:
            at = half + coarse.low
            between = (9.0 * (source[at] + source[at + 1]) - (source[at - 1] + source[at + 2])) / 16.0
            planes += [split_rows(source[at]), split_rows(between)]
        both = dot(table.get(table_ref, "tall", fine.index), jnp.concatenate(planes, 1))
        for k, half in enumerate(halves):
            emit(2 * half, both[:, 2 * k * LANES : (2 * k + 1) * LANES])
            emit(2 * half + 1, both[:, (2 * k + 1) * LANES : (2 * k + 2) * LANES])

    for fine, coarse in ((levels[2], levels[3]), (levels[1], levels[2])):
        sum_ref = sum_refs[fine.index - 1]
        source = sum_refs[coarse.index - 1]
        stretch(fine, coarse, source)

        def emit(at, value, fine=fine, sum_ref=sum_ref):
            plane = at + fine.low
            if 0 <= plane < fine.win[0]:
                sum_ref[plane] = sum_ref[plane] + value

        for half in range(-1, (fine.n[0] + fine.high + 1) // 2):
            prolong(fine, coarse, [half], source, emit)

    stretch(levels[0], levels[1], sum_refs[0])

    @pl.loop(0, levels[0].n[0] // 8)
    def _(group):
        def emit(at, value):
            out_ref[at] = (fine_ref[at] + value).astype(BF16)

        prolong(levels[0], levels[1], [4 * group + k for k in range(4)], sum_refs[0], emit)


def make_table(levels):
    table = Table()
    for level, fine in zip(levels[1:], levels[:3]):
        table.add(("send", level.index), send_lanes(level))
        table.add(("place", level.index), place_lanes(level))
        table.add(("tall", fine.index), prolong_rows(fine, level))
        table.add(("zed", fine.index), prolong_lanes(fine, level))
    return table


def ends_kernel(charges_ref, last_ref, first_ref):
    last_ref[...] = charges_ref[charges_ref.shape[0] - REACH :]
    first_ref[...] = charges_ref[:REACH]


def call(kernel, out_shape, args, scratch=(), spaces={}, flops=0, limit=12):
    specs = [pl.BlockSpec(memory_space=spaces.get(i, pltpu.VMEM)) for i in range(len(args))]
    single = not isinstance(out_shape, (list, tuple))
    outs = [out_shape] if single else list(out_shape)
    out_specs = [pl.BlockSpec(memory_space=pltpu.VMEM) for _ in outs]
    return pl.pallas_call(
        kernel,
        out_shape=out_shape,
        in_specs=specs,
        out_specs=out_specs[0] if single else out_specs,
        scratch_shapes=list(scratch),
        compiler_params=pltpu.CompilerParams(vmem_limit_bytes=limit << 20),
        cost_estimate=pl.CostEstimate(flops=flops, bytes_accessed=1 << 20, transcendentals=0),
    )(*args)


def shape(sizes, dtype):
    return jax.ShapeDtypeStruct(tuple(sizes), dtype)


def shifted(value, axis, by):
    count = lax.axis_size(axis)
    return lax.ppermute(value, axis, [(i, (i + by) % count) for i in range(count)])


def far_pair(value, axis):
    after = shifted(value, axis, 2)
    return [after] if lax.axis_size(axis) == 4 else [after, shifted(value, axis, -2)]


def z_pair(value, axis):
    half = value.shape[0] // 2
    if lax.axis_size(axis) == 2:
        return shifted(value, axis, 1)
    return jnp.concatenate([shifted(value[:half], axis, 1), shifted(value[half:], axis, -1)], 0)


def steps(charges, taps):
    levels = levels_of(charges.shape)
    table = make_table(levels)
    table_array = table.array()
    zero, coarse = levels[0], levels[1:]
    reach = REACH

    last, first = call(
        ends_kernel, [shape((reach, *charges.shape[1:]), BF16)] * 2, [charges], flops=1 << 20
    )
    x_prev = shifted(last, "gx", 1)
    x_next = shifted(first, "gx", -1)

    x_slab = shape((slab_planes(levels) * slab_pitch(levels), LANES), BF16)
    q, up, down, far = call(
        functools.partial(restrict_kernel, levels),
        [
            shape((sum(lv.win[0] * lv.rows for lv in coarse), LANES), F32),
            x_slab,
            x_slab,
            shape((far_groups(levels, levels[3].win[0]), SLAB, LANES), F32),
        ],
        [charges],
        flops=1 << 27,
    )
    band, lanes = call(
        functools.partial(bands_kernel, levels),
        [shape((16, 8 * TILE, 16 * TILE), BF16), shape((5 * LANES, 4 * LANES), BF16)],
        [taps.reshape(16, 17)],
        spaces={0: pltpu.SMEM},
        flops=1 << 26,
    )
    from_prev = shifted(up, "gx", 1)
    from_next = shifted(down, "gx", -1)
    far = far_pair(far, "gx")
    pieces = (x_prev, charges, x_next)
    y_prev = shifted(jnp.concatenate([x[:, -reach:] for x in pieces], 0), "gy", 1)
    y_next = shifted(jnp.concatenate([x[:, :reach] for x in pieces], 0), "gy", -1)

    y_slab = shape((slab_blocks(levels) * SLAB, LANES), BF16)
    r, up, down, far = call(
        functools.partial(rows_kernel, levels),
        [
            shape((sum(lv.full[0] * lv.rows for lv in coarse), LANES), F32),
            y_slab,
            y_slab,
            shape((far_groups(levels, levels[3].full[0]), SLAB, LANES), F32),
        ],
        [q, from_prev, from_next, *far],
        flops=1 << 25,
    )
    m_prev = shifted(up, "gy", 1)
    m_next = shifted(down, "gy", -1)
    far = far_pair(far, "gy")

    wide = jnp.concatenate([y_prev, jnp.concatenate(pieces, 0), y_next], 1)
    sides = call(
        halo_kernel,
        shape((2 * reach, wide.shape[0] * wide.shape[1]), BF16),
        [wide],
        flops=1 << 26,
    )
    halo = z_pair(sides, "gz")

    flat_rows = sum(level.span for level in coarse)
    flat, slabs = call(
        functools.partial(lanes_kernel, levels, table),
        [
            shape((flat_rows, LANES), F32),
            shape((2 * SLAB, 2 * flat_rows - levels[1].span), BF16),
        ],
        [r, m_prev, m_next, *far, table_array],
        flops=1 << 26,
    )
    slabs = z_pair(slabs, "gz")

    fine = call(
        functools.partial(fine_kernel, zero),
        shape(charges.shape, F32),
        [wide, halo, lanes, band],
        scratch=[
            pltpu.VMEM((*zero.inp, 4 * LANES), BF16),
            pltpu.VMEM((4, zero.out[1], zero.inp[0], LANES), BF16),
        ],
        flops=1 << 32,
        limit=24,
    )
    return call(
        functools.partial(coarse_kernel, levels, table),
        shape(charges.shape, BF16),
        [flat, slabs, lanes, band, table_array, fine],
        scratch=[pltpu.VMEM((*lv.inp, 4 * LANES), BF16) for lv in coarse]
        + [pltpu.VMEM((4, lv.out[1], lv.inp[0], LANES), BF16) for lv in coarse]
        + [pltpu.VMEM((*lv.out, LANES), F32) for lv in coarse],
        flops=1 << 31,
        limit=30,
    )


def solution(mesh):
    return jax.shard_map(
        steps,
        mesh=mesh,
        in_specs=(P("gx", "gy", "gz"), P()),
        out_specs=P("gx", "gy", "gz"),
        check_vma=False,
    )
```

```python
import functools

import jax
import jax.numpy as jnp
import numpy as np
from jax import lax
from jax.experimental import pallas as pl
from jax.experimental.pallas import tpu as pltpu
from jax.sharding import PartitionSpec as P


F32, BF16 = jnp.float32, jnp.bfloat16
REACH = 8
LANES = 128
TILE = 16
SLAB = 16
LOW, HIGH = (0, 1, 2, 2), (0, 2, 3, 3)
STENCIL = ((0, 1.0), (-1, 9 / 16), (1, 9 / 16), (-3, -1 / 16), (3, -1 / 16))


def up_to(value, step):
    return -(-value // step) * step


class Level:
    def __init__(self, index, block):
        self.index = index
        self.n = tuple(size >> index for size in block)
        self.low, self.high = LOW[index], HIGH[index]
        self.win = tuple(size + self.low + self.high for size in self.n)
        self.full = tuple(size + 2 * REACH for size in self.win)
        self.out = tuple(up_to(size, TILE) for size in self.win[:2])
        self.inp = tuple(size + TILE for size in self.out)
        self.rows = up_to(self.win[1], 8)
        self.lane = 0
        self.start = 0
        self.span = up_to(self.full[0] * self.inp[1], LANES)


def levels_of(block):
    levels = [Level(index, block) for index in range(4)]
    lane = 0
    for level in levels[1:]:
        level.lane = lane
        lane += level.win[2]
    levels[3].start = levels[2].span
    assert lane <= LANES and block[2] == LANES
    assert all(level.n[d] % 8 == 0 for level in levels for d in range(3))
    return levels


def own_lane(level, z):
    return (level.lane + z + level.low + REACH) % LANES


def stencil_of(offset, valid):
    size = jnp.abs(offset)
    weight = jnp.where(size == 0, 1.0, jnp.where(size == 1, 9 / 16, jnp.where(size == 3, -1 / 16, 0.0)))
    return jnp.where(valid, weight, 0.0).astype(BF16)


def restrict_rows(coarse, fine):
    fine_rows = fine.n[1] if fine.index == 0 else fine.rows
    row = lax.broadcasted_iota(jnp.int32, (coarse.rows, 2 * fine_rows), 0)
    col = lax.broadcasted_iota(jnp.int32, (coarse.rows, 2 * fine_rows), 1)
    col = jnp.where(col >= fine_rows, col - fine_rows, col)
    valid = (row < coarse.win[1]) & (col < fine.win[1])
    return stencil_of(col - fine.low - 2 * (row - coarse.low), valid)


def restrict_lanes(coarse, fine):
    k = lax.broadcasted_iota(jnp.int32, (2 * LANES, LANES), 0) % LANES
    lane = lax.broadcasted_iota(jnp.int32, (2 * LANES, LANES), 1)

    def place(level, lanes):
        return lanes if level.index == 0 else (lanes + (2 * LANES - level.lane - REACH)) % LANES

    k, lane = place(fine, k), place(coarse, lane)
    valid = (k < fine.win[2]) & (lane < coarse.win[2])
    return stencil_of(k - fine.low - 2 * (lane - coarse.low), valid)


def prolong_weights(fine_at):
    half = fine_at // 2
    if fine_at % 2 == 0:
        return ((half, 1.0),)
    return ((half, 9 / 16), (half + 1, 9 / 16), (half - 1, -1 / 16), (half + 2, -1 / 16))


def prolong_matrix(fine_count, fine_win, fine_low, coarse_count, coarse_low):
    matrix = np.zeros((fine_count, coarse_count))
    for row in range(fine_win):
        for at, weight in prolong_weights(row - fine_low):
            if 0 <= at + coarse_low < coarse_count:
                matrix[row, at + coarse_low] = weight
    return matrix


def prolong_rows(fine, coarse):
    matrix = prolong_matrix(fine.out[1], fine.win[1], fine.low, coarse.out[1], coarse.low)
    return np.concatenate([matrix, matrix], 1)


def prolong_lanes(fine, coarse):
    matrix = prolong_matrix(LANES, fine.win[2], fine.low, LANES, coarse.low).T
    return np.concatenate([matrix, matrix], 0)


def send_lanes(level):
    up, down = np.zeros((SLAB, LANES)), np.zeros((SLAB, LANES))
    for j in range(SLAB):
        s = level.n[2] - REACH + j
        if s < level.win[2]:
            up[j, own_lane(level, s - level.low)] = 1
        if j < level.low + level.high + REACH:
            down[j, own_lane(level, j - level.low)] = 1
    return np.concatenate([up, down], 0)


def place_lanes(level):
    from_prev, from_next = np.zeros((SLAB, LANES)), np.zeros((SLAB, LANES))
    for j in range(SLAB):
        if level.n[2] - REACH + j < level.win[2]:
            from_prev[j, (level.lane + j) % LANES] = 1
        at = j + REACH + level.n[2]
        if at < level.full[2]:
            from_next[j, (level.lane + at) % LANES] = 1
    return np.concatenate([from_prev, from_next] * (1 if level.index == 1 else 2), 0)


def dot(a, b, dims=((1,), (0,))):
    return lax.dot_general(a, b, (dims, ((), ())), preferred_element_type=F32)


def split_rows(x):
    high = x.astype(BF16).astype(F32)
    return jnp.concatenate([high, x - high], 0).astype(BF16)


def split_lanes(x):
    high = x.astype(BF16).astype(F32)
    return jnp.concatenate([high, x - high], 1).astype(BF16)


class Table:
    def __init__(self):
        self.parts, self.places, self.count = [], {}, 0

    def add(self, key, matrix):
        rows, cols = matrix.shape
        padded = np.zeros((up_to(rows, TILE), LANES), np.float32)
        padded[:rows, :cols] = matrix
        self.places[key] = (self.count, rows, cols)
        self.parts.append(padded)
        self.count += padded.shape[0]

    def array(self):
        return jnp.asarray(np.concatenate(self.parts, 0), BF16)

    def get(self, ref, *key):
        start, rows, cols = self.places[key]
        return ref[start : start + rows, :cols]


def pad_rows(x, rows):
    if x.shape[0] == rows:
        return x
    return jnp.concatenate([x, jnp.zeros((rows - x.shape[0], x.shape[1]), x.dtype)], 0)


def total(terms):
    return functools.reduce(lambda a, b: a + b, terms)


def bands_kernel(levels, taps_ref, band_ref, lanes_ref):
    row = lax.broadcasted_iota(jnp.int32, (8 * TILE, 16 * TILE), 0)
    col = lax.broadcasted_iota(jnp.int32, (8 * TILE, 16 * TILE), 1)
    offset = jnp.where(row % 8 == col // 32, col % 32 - row // 8, -1)

    @pl.loop(0, 16)
    def _(which):
        matrix = jnp.zeros(offset.shape, F32)
        for tap in range(17):
            matrix = jnp.where(offset == tap, taps_ref[which, tap], matrix)
        band_ref[which] = matrix.astype(BF16)

    for level in levels:
        first, count = lane_rows(level)
        k = lax.broadcasted_iota(jnp.int32, (count, LANES), 0)
        z_out = lax.broadcasted_iota(jnp.int32, (count, LANES), 1)
        if level.index == 0:
            n = level.n[2]
            z_in = jnp.where(k < n, k + REACH, jnp.where(k < n + REACH, k - n, k))
            valid = k < n + 2 * REACH
        else:
            z_in = (k + (LANES - level.lane)) % LANES
            valid = (z_in < level.full[2]) & (z_out < level.win[2])
        offset_z = jnp.where(valid, z_in - z_out, -1)
        for term in range(4):
            matrix = jnp.zeros(offset_z.shape, F32)
            for tap in range(17):
                matrix = jnp.where(offset_z == tap, taps_ref[4 * level.index + term, tap], matrix)
            lanes_ref[first : first + count, term_lanes(term)] = matrix.astype(BF16)


def lane_rows(level):
    return (0, 2 * LANES) if level.index == 0 else ((level.index + 1) * LANES, LANES)


def term_lanes(term):
    return slice(term * LANES, (term + 1) * LANES)


def plane_at(levels, level, which, rows):
    first = 0
    for other in levels[1:]:
        sizes = (other.win[0], other.rows) if rows == "own" else (other.full[0], other.rows)
        if other is level:
            return slice(first + which * sizes[1], first + (which + 1) * sizes[1])
        first += sizes[0] * sizes[1]
    return first


def halves_of(x):
    high = x.astype(BF16).astype(F32)
    return high, x - high


def restrict_kernel(
    levels, charges_ref, q_ref, up_ref, down_ref, far_ref
):
    for level, fine in zip(levels[1:], levels[:3]):
        by_rows, by_lanes = restrict_rows(level, fine), restrict_lanes(level, fine)
        for at in range(level.win[0]):
            terms = {}
            for offset, weight in STENCIL:
                plane = 2 * (at - level.low) + offset + fine.low
                if 0 <= plane < fine.win[0]:
                    if fine.index == 0:
                        value = charges_ref[plane].astype(F32)
                    else:
                        value = q_ref[plane_at(levels, fine, plane, "own")]
                    terms.setdefault(weight, []).append(value)
            value = total([total(group) * weight for weight, group in terms.items()])
            value = dot(by_rows, split_rows(value))
            value = dot(split_lanes(value), by_lanes)
            q_ref[plane_at(levels, level, at, "own")] = value
    high_rows, rest_rows = levels[1].rows, levels[2].rows
    pitch = slab_pitch(levels)
    planes = slab_planes(levels)
    for j in range(planes):
        for slab_ref, bases in ((up_ref, [lv.n[0] - REACH for lv in levels[1:]]), (down_ref, [0] * 3)):
            highs, rests = [], [jnp.zeros((rest_rows, LANES), F32)]
            for level, base in zip(levels[1:], bases):
                if base + j < level.win[0]:
                    high, rest = halves_of(q_ref[plane_at(levels, level, base + j, "own")])
                    highs.append(pad_rows(high, high_rows))
                    if level.index > 1:
                        rests.append(pad_rows(rest, rest_rows))
            rest = jnp.concatenate([jnp.zeros((rest_rows, LANES), F32), total(rests)], 0)
            value = pad_rows(total(highs), pitch) + rest
            slab_ref[j * pitch : (j + 1) * pitch] = value.astype(BF16)
    last = levels[3]
    pack_far(
        levels,
        far_ref,
        [q_ref[plane_at(levels, last, at, "own")] for at in range(last.win[0])],
    )


def slab_planes(levels):
    return max(level.low + level.high + REACH for level in levels[1:])


def slab_pitch(levels):
    return up_to(max(levels[1].rows, 2 * levels[2].rows), TILE)


def rest_block(levels, plane):
    spare = levels[1].full[0] - levels[2].full[0]
    if plane < spare:
        return levels[2].full[0] + plane, 0
    return levels[1].full[0] + (plane - spare) // 2, LANES // 2 * ((plane - spare) % 2)


def slab_blocks(levels):
    return rest_block(levels, levels[2].full[0] - 1)[0] + 1


def turned(x, lanes):
    return pltpu.roll(x, lanes % LANES, 1) if lanes % LANES else x


def far_groups(levels, planes):
    return -(-planes // (LANES // levels[3].win[2]))


def pack_far(levels, far_ref, planes):
    width = levels[3].win[2]
    per = LANES // width
    for group in range(far_ref.shape[0]):
        members = planes[per * group : per * group + per]
        far_ref[group] = total([turned(x, width * k) for k, x in enumerate(members)])


def unpack_far(levels, far_ref, at):
    width = levels[3].win[2]
    per = LANES // width
    return turned(far_ref[at // per], LANES - width * (at % per))


def lane_masks(levels):
    lane = lax.broadcasted_iota(jnp.int32, (8, LANES), 1)
    masks = []
    for level in levels[1:]:
        at = (lane + (2 * LANES - level.lane - REACH)) % LANES
        masks.append((at < level.win[2])[:1])
    return masks


def rows_kernel(levels, q_ref, prev_ref, next_ref, far_prev_ref, *refs):
    far_next_ref = far_prev_ref if len(refs) == 4 else refs[0]
    x_ref, up_ref, down_ref, far_ref = refs[-4:]
    count, pitch, rest_rows = slab_planes(levels), slab_pitch(levels), levels[2].rows
    masks = lane_masks(levels)
    coarsest = []

    def received(ref, at, level):
        slab = ref[at * pitch : (at + 1) * pitch].astype(F32)
        high = slab[: level.rows]
        return high if level.index == 1 else high + slab[rest_rows : rest_rows + level.rows]

    blocks = {True: {}, False: {}}
    for at in range(levels[1].full[0]):
        for level, mask in zip(levels[1:], masks):
            if at >= level.full[0]:
                continue
            n = level.n[0]
            terms = []
            if 0 <= at - REACH < level.win[0]:
                terms.append(q_ref[plane_at(levels, level, at - REACH, "own")])
            if at < count and at - REACH + n < level.win[0]:
                terms.append(received(prev_ref, at, level))
            if 0 <= at - REACH - n < count:
                terms.append(received(next_ref, at - REACH - n, level))
            if level.index == 3:
                if at - REACH + 2 * n < level.win[0]:
                    terms.append(unpack_far(levels, far_prev_ref, at - REACH + 2 * n))
                if at - REACH - 2 * n >= 0:
                    terms.append(unpack_far(levels, far_next_ref, at - REACH - 2 * n))
            value = jnp.where(mask, total(terms), 0.0)
            x_ref[plane_at(levels, level, at, "full")] = value
            first = level.n[1] - REACH
            for is_up, rows in ((True, value[first : first + SLAB]), (False, value[:SLAB])):
                high, rest = halves_of(rows)
                blocks[is_up].setdefault(at, []).append(high)
                if level.index > 1:
                    block, lanes = rest_block(levels, at)
                    blocks[is_up].setdefault(block, []).append(turned(rest, lanes))
            if level.index == 3:
                coarsest.append(value)
    for is_up, slab_ref in ((True, up_ref), (False, down_ref)):
        for block, parts in blocks[is_up].items():
            slab_ref[block * SLAB : (block + 1) * SLAB] = total(parts).astype(BF16)
    pack_far(levels, far_ref, coarsest)


def lanes_kernel(levels, table, x_ref, prev_ref, next_ref, far_prev_ref, *refs):
    far_next_ref = far_prev_ref if len(refs) == 5 else refs[0]
    table_ref, flat_refs, slab_refs = refs[-5], refs[-4:-2], refs[-2:]

    def block_of(ref, block):
        return ref[block * SLAB : (block + 1) * SLAB].astype(F32)

    def received(ref, at, level):
        high = block_of(ref, at)
        if level.index == 1:
            return high
        block, lanes = rest_block(levels, at)
        return high + turned(block_of(ref, block), LANES - lanes)

    for level, mask in zip(levels[1:], lane_masks(levels)):
        blocks, step = level.inp[1] // 8, level.n[1] // 8
        flat_ref = flat_refs[level.index > 1]
        for at in range(level.full[0]):
            own = x_ref[plane_at(levels, level, at, "full")]
            slabs = [received(prev_ref, at, level), received(next_ref, at, level)]
            if level.index == 3:
                slabs += [unpack_far(levels, ref, at) for ref in (far_prev_ref, far_next_ref)]
            parts = []
            for block in range(blocks):
                terms = []
                if 0 <= block - 1 < level.rows // 8:
                    terms.append(own[8 * block - 8 : 8 * block])
                places = [block, block - 1 - step, block - 1 + 2 * step, block - 1 - 2 * step]
                for slab, place in zip(slabs, places):
                    if 0 <= place < SLAB // 8:
                        terms.append(slab[8 * place : 8 * place + 8])
                parts.append(total(terms) if terms else jnp.zeros((8, LANES), F32))
            value = jnp.where(mask, jnp.concatenate(parts, 0), 0.0)
            first = level.start + at * level.inp[1]
            flat_ref[first : first + level.inp[1]] = value
        used = level.start + level.full[0] * level.inp[1]
        last = level.start + level.span
        if used < last:
            flat_ref[used:last] = jnp.zeros((last - used, LANES), F32)
    shift = levels[2].span + levels[3].span
    for level in levels[1:]:
        flat_ref, slab_ref = flat_refs[level.index > 1], slab_refs[level.index > 1]
        send = table.get(table_ref, "send", level.index)
        for first in range(level.start, level.start + level.span, 512):
            stop = min(first + 512, level.start + level.span)
            high, rest = halves_of(flat_ref[first:stop])
            slab_ref[:, first:stop] = dot(send, high.astype(BF16), ((1,), (1,))).astype(BF16)
            if level.index > 1:
                slab_ref[:, first + shift : stop + shift] = dot(
                    send, rest.astype(BF16), ((1,), (1,))
                ).astype(BF16)


def halo_kernel(wide_ref, out_ref):
    planes, rows, count = wide_ref.shape
    row = lax.broadcasted_iota(jnp.int32, (2 * REACH, count), 0)
    lane = lax.broadcasted_iota(jnp.int32, (2 * REACH, count), 1)
    send = jnp.where(lane == (row + (count - REACH)) % count, 1.0, 0.0).astype(BF16)
    step = 8
    for first in range(0, planes, step):
        chunk = wide_ref[first : first + step].reshape(step * rows, LANES)
        out_ref[:, first * rows : (first + step) * rows] = dot(send, chunk, ((1,), (1,))).astype(BF16)


def two_passes(level, band, first_ref, second_ref, put):
    def parts_of(result):
        parts = [result[:, :LANES], result[:, LANES:]]
        return jnp.concatenate([x.reshape(TILE, 8, LANES) for x in parts], 1)

    def along_y(pair):
        for block in range(level.out[1] // TILE):
            for term in range(4):
                halves = [
                    first_ref[
                        slice(pair * 16 + 8 * half, pair * 16 + 8 * half + 8),
                        TILE * block : TILE * block + 32,
                        term_lanes(term),
                    ].reshape(256, LANES)
                    for half in range(2)
                ]
                result = dot(band(term), jnp.concatenate(halves, 1))
                second_ref[
                    term, TILE * block : TILE * (block + 1), slice(pair * 16, pair * 16 + 16)
                ] = parts_of(result).astype(BF16)

    def along_x(pair):
        for block in range(level.out[0] // TILE):
            result = None
            for term in range(4):
                halves = [
                    second_ref[
                        term, slice(pair * 16 + 8 * half, pair * 16 + 8 * half + 8), TILE * block : TILE * block + 32
                    ].reshape(256, LANES)
                    for half in range(2)
                ]
                part = dot(band(term), jnp.concatenate(halves, 1))
                result = part if result is None else result + part
            put(block, pair, parts_of(result))

    for pair in range(level.inp[0] // 16):
        along_y(pair)
    for pair in range(level.out[1] // 16):
        along_x(pair)


def fine_kernel(level, wide_ref, halo_ref, lanes_ref, band_ref, out_ref, first_ref, second_ref):
    rows, step = level.inp[1], 16
    row = lax.broadcasted_iota(jnp.int32, (2 * REACH, LANES), 0)
    lane = lax.broadcasted_iota(jnp.int32, (2 * REACH, LANES), 1)
    place = jnp.where(lane == row, 1.0, 0.0).astype(BF16)

    @pl.loop(0, level.inp[0] // step)
    def _(chunk):
        where = pl.ds(pl.multiple_of(chunk * step * rows, LANES), step * rows)
        sides = dot(halo_ref[:, where], place, ((0,), (0,))).astype(BF16)
        here = wide_ref[pl.ds(chunk * step, step)].reshape(step * rows, LANES)
        result = dot(jnp.concatenate([here, sides], 1), lanes_ref[: 2 * LANES])
        first_ref[pl.ds(chunk * step, step)] = result.astype(BF16).reshape(step, rows, 4 * LANES)

    def put(block, pair, value):
        out_ref[TILE * block : TILE * (block + 1), slice(pair * 16, pair * 16 + 16)] = value

    two_passes(level, lambda term: band_ref[term], first_ref, second_ref, put)


def level_passes(levels, level, table, flat_ref, slab_ref, lanes_ref, band_ref, table_ref, first_ref, second_ref, sum_ref):
    shift = levels[2].span + levels[3].span
    rows, step = level.inp[1], 4
    first_lane, _ = lane_rows(level)
    place = table.get(table_ref, "place", level.index)
    for plane in range(0, level.full[0], step):
        count = min(step, level.full[0] - plane)
        if (count * rows) % LANES:
            count += 1
        start, stop = level.start + plane * rows, level.start + (plane + count) * rows
        slab = slab_ref[:, start:stop]
        if level.index > 1:
            slab = jnp.concatenate([slab, slab_ref[:, start + shift : stop + shift]], 0)
        value = flat_ref[start:stop] + dot(slab, place, ((0,), (0,)))
        result = dot(value.astype(BF16), lanes_ref[first_lane : first_lane + LANES])
        first_ref[plane : plane + count] = result.astype(BF16).reshape(count, rows, 4 * LANES)
    rest = level.inp[0] - plane - count
    if rest > 0:
        first_ref[plane + count :] = jnp.zeros((rest, rows, 4 * LANES), BF16)

    def put(block, pair, value):
        sum_ref[TILE * block : TILE * (block + 1), slice(pair * 16, pair * 16 + 16)] = value

    base = 4 * level.index
    two_passes(level, lambda term: band_ref[base + term], first_ref, second_ref, put)


def middle_kernel(levels, table, flat_ref, slab_ref, lanes_ref, band_ref, table_ref, sum_ref, first_ref, second_ref):
    level_passes(levels, levels[1], table, flat_ref, slab_ref, lanes_ref, band_ref, table_ref, first_ref, second_ref, sum_ref)


def coarse_kernel(levels, table, flat_ref, slab_ref, lanes_ref, band_ref, table_ref, middle_ref, fine_ref, *refs):
    out_ref, first_refs, second_refs, sum_refs = refs[0], refs[1:3], refs[3:5], refs[5:8]
    for level in (levels[3], levels[2]):
        which = level.index - 2
        level_passes(
            levels, level, table, flat_ref, slab_ref, lanes_ref, band_ref, table_ref,
            first_refs[which], second_refs[which], sum_refs[level.index - 1],
        )

    def stretch(fine, coarse, source):
        planes, rows, _ = source.shape
        for first in range(0, coarse.win[0], 4):
            count = min(4, planes - first)
            value = split_lanes(source[first : first + count].reshape(count * rows, LANES))
            value = dot(value, table.get(table_ref, "zed", fine.index))
            source[first : first + count] = value.reshape(count, rows, LANES)

    def prolong(fine, coarse, halves, source, emit):
        planes = []
        for half in halves:
            at = half + coarse.low
            between = (9.0 * (source[at] + source[at + 1]) - (source[at - 1] + source[at + 2])) / 16.0
            planes += [split_rows(source[at]), split_rows(between)]
        both = dot(table.get(table_ref, "tall", fine.index), jnp.concatenate(planes, 1))
        for k, half in enumerate(halves):
            emit(2 * half, both[:, 2 * k * LANES : (2 * k + 1) * LANES])
            emit(2 * half + 1, both[:, (2 * k + 1) * LANES : (2 * k + 2) * LANES])

    for fine, coarse in ((levels[2], levels[3]), (levels[1], levels[2])):
        sum_ref = sum_refs[fine.index - 1]
        source = sum_refs[coarse.index - 1]
        stretch(fine, coarse, source)

        def emit(at, value, fine=fine, sum_ref=sum_ref):
            plane = at + fine.low
            if 0 <= plane < fine.win[0]:
                sum_ref[plane] = (middle_ref if fine.index == 1 else sum_ref)[plane] + value

        for half in range(-1, (fine.n[0] + fine.high + 1) // 2):
            prolong(fine, coarse, [half], source, emit)

    stretch(levels[0], levels[1], sum_refs[0])

    @pl.loop(0, levels[0].n[0] // 8)
    def _(group):
        def emit(at, value):
            out_ref[at] = (fine_ref[at] + value).astype(BF16)

        prolong(levels[0], levels[1], [4 * group + k for k in range(4)], sum_refs[0], emit)


def make_table(levels):
    table = Table()
    for level, fine in zip(levels[1:], levels[:3]):
        table.add(("send", level.index), send_lanes(level))
        table.add(("place", level.index), place_lanes(level))
        table.add(("tall", fine.index), prolong_rows(fine, level))
        table.add(("zed", fine.index), prolong_lanes(fine, level))
    return table


def ends_kernel(charges_ref, last_ref, first_ref):
    last_ref[...] = charges_ref[charges_ref.shape[0] - REACH :]
    first_ref[...] = charges_ref[:REACH]


def call(kernel, out_shape, args, scratch=(), spaces={}, flops=0, limit=12):
    specs = [pl.BlockSpec(memory_space=spaces.get(i, pltpu.VMEM)) for i in range(len(args))]
    single = not isinstance(out_shape, (list, tuple))
    outs = [out_shape] if single else list(out_shape)
    out_specs = [pl.BlockSpec(memory_space=pltpu.VMEM) for _ in outs]
    return pl.pallas_call(
        kernel,
        out_shape=out_shape,
        in_specs=specs,
        out_specs=out_specs[0] if single else out_specs,
        scratch_shapes=list(scratch),
        compiler_params=pltpu.CompilerParams(vmem_limit_bytes=limit << 20),
        cost_estimate=pl.CostEstimate(flops=flops, bytes_accessed=1 << 20, transcendentals=0),
    )(*args)


def shape(sizes, dtype):
    return jax.ShapeDtypeStruct(tuple(sizes), dtype)


def shifted(value, axis, by):
    count = lax.axis_size(axis)
    return lax.ppermute(value, axis, [(i, (i + by) % count) for i in range(count)])


def far_pair(value, axis):
    after = shifted(value, axis, 2)
    return [after] if lax.axis_size(axis) == 4 else [after, shifted(value, axis, -2)]


def z_pair(value, axis):
    half = value.shape[0] // 2
    if lax.axis_size(axis) == 2:
        return shifted(value, axis, 1)
    return jnp.concatenate([shifted(value[:half], axis, 1), shifted(value[half:], axis, -1)], 0)


def steps(charges, taps):
    levels = levels_of(charges.shape)
    table = make_table(levels)
    table_array = table.array()
    zero, coarse = levels[0], levels[1:]
    reach = REACH

    last, first = call(
        ends_kernel, [shape((reach, *charges.shape[1:]), BF16)] * 2, [charges], flops=1 << 20
    )
    x_prev = shifted(last, "gx", 1)
    x_next = shifted(first, "gx", -1)

    x_slab = shape((slab_planes(levels) * slab_pitch(levels), LANES), BF16)
    q, up, down, far = call(
        functools.partial(restrict_kernel, levels),
        [
            shape((sum(lv.win[0] * lv.rows for lv in coarse), LANES), F32),
            x_slab,
            x_slab,
            shape((far_groups(levels, levels[3].win[0]), SLAB, LANES), F32),
        ],
        [charges],
        flops=1 << 27,
    )
    band, lanes = call(
        functools.partial(bands_kernel, levels),
        [shape((16, 8 * TILE, 16 * TILE), BF16), shape((5 * LANES, 4 * LANES), BF16)],
        [taps.reshape(16, 17)],
        spaces={0: pltpu.SMEM},
        flops=1 << 26,
    )
    from_prev = shifted(up, "gx", 1)
    from_next = shifted(down, "gx", -1)
    far = far_pair(far, "gx")
    pieces = (x_prev, charges, x_next)
    y_prev = shifted(jnp.concatenate([x[:, -reach:] for x in pieces], 0), "gy", 1)
    y_next = shifted(jnp.concatenate([x[:, :reach] for x in pieces], 0), "gy", -1)

    y_slab = shape((slab_blocks(levels) * SLAB, LANES), BF16)
    r, up, down, far = call(
        functools.partial(rows_kernel, levels),
        [
            shape((sum(lv.full[0] * lv.rows for lv in coarse), LANES), F32),
            y_slab,
            y_slab,
            shape((far_groups(levels, levels[3].full[0]), SLAB, LANES), F32),
        ],
        [q, from_prev, from_next, *far],
        flops=1 << 25,
    )
    m_prev = shifted(up, "gy", 1)
    m_next = shifted(down, "gy", -1)
    far = far_pair(far, "gy")

    wide = jnp.concatenate([y_prev, jnp.concatenate(pieces, 0), y_next], 1)
    sides = call(
        halo_kernel,
        shape((2 * reach, wide.shape[0] * wide.shape[1]), BF16),
        [wide],
        flops=1 << 26,
    )
    halo = z_pair(sides, "gz")

    spans = (coarse[0].span, coarse[1].span + coarse[2].span)
    *flats, slab_one, slab_two = call(
        functools.partial(lanes_kernel, levels, table),
        [shape((span, LANES), F32) for span in spans]
        + [shape((2 * SLAB, count), BF16) for count in (spans[0], 2 * spans[1])],
        [r, m_prev, m_next, *far, table_array],
        flops=1 << 26,
    )
    slab_one = z_pair(slab_one, "gz")
    slab_two = z_pair(slab_two, "gz")

    fine = call(
        functools.partial(fine_kernel, zero),
        shape(charges.shape, F32),
        [wide, halo, lanes, band],
        scratch=[
            pltpu.VMEM((*zero.inp, 4 * LANES), BF16),
            pltpu.VMEM((4, zero.out[1], zero.inp[0], LANES), BF16),
        ],
        flops=1 << 32,
        limit=20,
    )
    slab_one, fine = lax.optimization_barrier((slab_one, fine))

    def scratch(some):
        return [pltpu.VMEM((*lv.inp, 4 * LANES), BF16) for lv in some] + [
            pltpu.VMEM((4, lv.out[1], lv.inp[0], LANES), BF16) for lv in some
        ]

    middle = call(
        functools.partial(middle_kernel, levels, table),
        shape((*coarse[0].out, LANES), F32),
        [flats[0], slab_one, lanes, band, table_array],
        scratch=scratch(coarse[:1]),
        flops=1 << 31,
        limit=16,
    )
    return call(
        functools.partial(coarse_kernel, levels, table),
        shape(charges.shape, BF16),
        [flats[1], slab_two, lanes, band, table_array, middle, fine],
        scratch=scratch(coarse[1:]) + [pltpu.VMEM((*lv.out, LANES), F32) for lv in coarse],
        flops=1 << 30,
        limit=16,
    )


def solution(mesh):
    return jax.shard_map(
        steps,
        mesh=mesh,
        in_specs=(P("gx", "gy", "gz"), P()),
        out_specs=P("gx", "gy", "gz"),
        check_vma=False,
    )
```

```python
import functools

import jax
import jax.numpy as jnp
import numpy as np
from jax import lax
from jax.experimental import pallas as pl
from jax.experimental.pallas import tpu as pltpu
from jax.sharding import PartitionSpec as P


F32, BF16 = jnp.float32, jnp.bfloat16
REACH = 8
LANES = 128
TILE = 16
SLAB = 16
LOW, HIGH = (0, 1, 2, 2), (0, 2, 3, 3)
STENCIL = ((0, 1.0), (-1, 9 / 16), (1, 9 / 16), (-3, -1 / 16), (3, -1 / 16))


def up_to(value, step):
    return -(-value // step) * step


class Level:
    def __init__(self, index, block):
        self.index = index
        self.n = tuple(size >> index for size in block)
        self.low, self.high = LOW[index], HIGH[index]
        self.win = tuple(size + self.low + self.high for size in self.n)
        self.full = tuple(size + 2 * REACH for size in self.win)
        self.out = tuple(up_to(size, TILE) for size in self.win[:2])
        self.inp = tuple(size + TILE for size in self.out)
        self.rows = up_to(self.win[1], 8)
        self.lane = 0
        self.start = self.flat = 0
        self.sent_rows = up_to(self.full[1], 8)
        self.span = up_to(self.full[0] * self.sent_rows, LANES)
        self.sent = up_to(self.low + self.high + REACH, 4)


def levels_of(block):
    levels = [Level(index, block) for index in range(4)]
    lane = 0
    for level in levels[1:]:
        level.lane = lane
        lane += level.win[2]
    levels[3].start = levels[2].span
    levels[3].flat = levels[2].full[0] * levels[2].inp[1]
    assert lane <= LANES and block[2] == LANES
    assert all(level.n[d] % 8 == 0 for level in levels for d in range(3))
    return levels


def own_lane(level, z):
    return (level.lane + z + level.low + REACH) % LANES


def stencil_of(offset, valid):
    size = jnp.abs(offset)
    weight = jnp.where(size == 0, 1.0, jnp.where(size == 1, 9 / 16, jnp.where(size == 3, -1 / 16, 0.0)))
    return jnp.where(valid, weight, 0.0).astype(BF16)


def restrict_rows(coarse, fine):
    fine_rows = fine.n[1] if fine.index == 0 else fine.rows
    row = lax.broadcasted_iota(jnp.int32, (coarse.rows, 2 * fine_rows), 0)
    col = lax.broadcasted_iota(jnp.int32, (coarse.rows, 2 * fine_rows), 1)
    col = jnp.where(col >= fine_rows, col - fine_rows, col)
    valid = (row < coarse.win[1]) & (col < fine.win[1])
    return stencil_of(col - fine.low - 2 * (row - coarse.low), valid)


def restrict_lanes(coarse, fine):
    k = lax.broadcasted_iota(jnp.int32, (2 * LANES, LANES), 0) % LANES
    lane = lax.broadcasted_iota(jnp.int32, (2 * LANES, LANES), 1)

    def place(level, lanes):
        return lanes if level.index == 0 else (lanes + (2 * LANES - level.lane - REACH)) % LANES

    k, lane = place(fine, k), place(coarse, lane)
    valid = (k < fine.win[2]) & (lane < coarse.win[2])
    return stencil_of(k - fine.low - 2 * (lane - coarse.low), valid)


def prolong_weights(fine_at):
    half = fine_at // 2
    if fine_at % 2 == 0:
        return ((half, 1.0),)
    return ((half, 9 / 16), (half + 1, 9 / 16), (half - 1, -1 / 16), (half + 2, -1 / 16))


def prolong_matrix(fine_count, fine_win, fine_low, coarse_count, coarse_low):
    matrix = np.zeros((fine_count, coarse_count))
    for row in range(fine_win):
        for at, weight in prolong_weights(row - fine_low):
            if 0 <= at + coarse_low < coarse_count:
                matrix[row, at + coarse_low] = weight
    return matrix


def prolong_rows(fine, coarse):
    matrix = prolong_matrix(fine.out[1], fine.win[1], fine.low, coarse.out[1], coarse.low)
    return np.concatenate([matrix, matrix], 1)


def prolong_lanes(fine, coarse):
    matrix = prolong_matrix(LANES, fine.win[2], fine.low, LANES, coarse.low).T
    return np.concatenate([matrix, matrix], 0)


def send_lanes(level):
    up, down = np.zeros((level.sent, LANES)), np.zeros((level.sent, LANES))
    for j in range(level.sent):
        s = level.n[2] - REACH + j
        if s < level.win[2]:
            up[j, own_lane(level, s - level.low)] = 1
        if j < level.low + level.high + REACH:
            down[j, own_lane(level, j - level.low)] = 1
    return np.concatenate([up, down], 0)


def place_lanes(level):
    from_prev, from_next = np.zeros((level.sent, LANES)), np.zeros((level.sent, LANES))
    for j in range(level.sent):
        if level.n[2] - REACH + j < level.win[2]:
            from_prev[j, (level.lane + j) % LANES] = 1
        at = j + REACH + level.n[2]
        if at < level.full[2]:
            from_next[j, (level.lane + at) % LANES] = 1
    return np.concatenate([from_prev, from_next] * (1 if level.index == 1 else 2), 0)


def dot(a, b, dims=((1,), (0,))):
    return lax.dot_general(a, b, (dims, ((), ())), preferred_element_type=F32)


def split_rows(x):
    high = x.astype(BF16).astype(F32)
    return jnp.concatenate([high, x - high], 0).astype(BF16)


def split_lanes(x):
    high = x.astype(BF16).astype(F32)
    return jnp.concatenate([high, x - high], 1).astype(BF16)


class Table:
    def __init__(self):
        self.parts, self.places, self.count = [], {}, 0

    def add(self, key, matrix):
        rows, cols = matrix.shape
        padded = np.zeros((up_to(rows, TILE), LANES), np.float32)
        padded[:rows, :cols] = matrix
        self.places[key] = (self.count, rows, cols)
        self.parts.append(padded)
        self.count += padded.shape[0]

    def array(self):
        return jnp.asarray(np.concatenate(self.parts, 0), BF16)

    def get(self, ref, *key):
        start, rows, cols = self.places[key]
        return ref[start : start + rows, :cols]


def pad_rows(x, rows):
    if x.shape[0] == rows:
        return x
    return jnp.concatenate([x, jnp.zeros((rows - x.shape[0], x.shape[1]), x.dtype)], 0)


def total(terms):
    return functools.reduce(lambda a, b: a + b, terms)


def bands_kernel(levels, taps_ref, band_ref, lanes_ref):
    row = lax.broadcasted_iota(jnp.int32, (8 * TILE, 16 * TILE), 0)
    col = lax.broadcasted_iota(jnp.int32, (8 * TILE, 16 * TILE), 1)
    offset = jnp.where(row % 8 == col // 32, col % 32 - row // 8, -1)

    @pl.loop(0, 16)
    def _(which):
        matrix = jnp.zeros(offset.shape, F32)
        for tap in range(17):
            matrix = jnp.where(offset == tap, taps_ref[which, tap], matrix)
        band_ref[which] = matrix.astype(BF16)

    for level in levels:
        first, count = lane_rows(level)
        k = lax.broadcasted_iota(jnp.int32, (count, LANES), 0)
        z_out = lax.broadcasted_iota(jnp.int32, (count, LANES), 1)
        if level.index == 0:
            n = level.n[2]
            z_in = jnp.where(k < n, k + REACH, jnp.where(k < n + REACH, k - n, k))
            valid = k < n + 2 * REACH
        else:
            z_in = (k + (LANES - level.lane)) % LANES
            valid = (z_in < level.full[2]) & (z_out < level.win[2])
        offset_z = jnp.where(valid, z_in - z_out, -1)
        for term in range(4):
            matrix = jnp.zeros(offset_z.shape, F32)
            for tap in range(17):
                matrix = jnp.where(offset_z == tap, taps_ref[4 * level.index + term, tap], matrix)
            lanes_ref[first : first + count, term_lanes(term)] = matrix.astype(BF16)


def lane_rows(level):
    return (0, 2 * LANES) if level.index == 0 else ((level.index + 1) * LANES, LANES)


def term_lanes(term):
    return slice(term * LANES, (term + 1) * LANES)


def plane_at(levels, level, which, rows):
    first = 0
    for other in levels[1:]:
        sizes = (other.win[0], other.rows) if rows == "own" else (other.full[0], other.rows)
        if other is level:
            return slice(first + which * sizes[1], first + (which + 1) * sizes[1])
        first += sizes[0] * sizes[1]
    return first


def halves_of(x):
    high = x.astype(BF16).astype(F32)
    return high, x - high


def restrict_kernel(
    levels, charges_ref, q_ref, up_ref, down_ref, far_ref
):
    for level, fine in zip(levels[1:], levels[:3]):
        by_rows, by_lanes = restrict_rows(level, fine), restrict_lanes(level, fine)
        for at in range(level.win[0]):
            terms = {}
            for offset, weight in STENCIL:
                plane = 2 * (at - level.low) + offset + fine.low
                if 0 <= plane < fine.win[0]:
                    if fine.index == 0:
                        value = charges_ref[plane].astype(F32)
                    else:
                        value = q_ref[plane_at(levels, fine, plane, "own")]
                    terms.setdefault(weight, []).append(value)
            value = total([total(group) * weight for weight, group in terms.items()])
            value = dot(by_rows, split_rows(value))
            value = dot(split_lanes(value), by_lanes)
            q_ref[plane_at(levels, level, at, "own")] = value
    high_rows, rest_rows = levels[1].rows, levels[2].rows
    pitch = slab_pitch(levels)
    planes = slab_planes(levels)
    for j in range(planes):
        for slab_ref, bases in ((up_ref, [lv.n[0] - REACH for lv in levels[1:]]), (down_ref, [0] * 3)):
            highs, rests = [], [jnp.zeros((rest_rows, LANES), F32)]
            for level, base in zip(levels[1:], bases):
                if base + j < level.win[0]:
                    high, rest = halves_of(q_ref[plane_at(levels, level, base + j, "own")])
                    highs.append(pad_rows(high, high_rows))
                    if level.index > 1:
                        rests.append(pad_rows(rest, rest_rows))
            rest = jnp.concatenate([jnp.zeros((rest_rows, LANES), F32), total(rests)], 0)
            value = pad_rows(total(highs), pitch) + rest
            slab_ref[j * pitch : (j + 1) * pitch] = value.astype(BF16)
    last = levels[3]
    pack_far(
        levels,
        far_ref,
        [q_ref[plane_at(levels, last, at, "own")] for at in range(last.win[0])],
    )


def slab_planes(levels):
    return max(level.low + level.high + REACH for level in levels[1:])


def slab_pitch(levels):
    return up_to(max(levels[1].rows, 2 * levels[2].rows), TILE)


def rest_block(levels, plane):
    spare = levels[1].full[0] - levels[2].full[0]
    if plane < spare:
        return levels[2].full[0] + plane, 0
    return levels[1].full[0] + (plane - spare) // 2, LANES // 2 * ((plane - spare) % 2)


def slab_blocks(levels):
    return rest_block(levels, levels[2].full[0] - 1)[0] + 1


def turned(x, lanes):
    return pltpu.roll(x, lanes % LANES, 1) if lanes % LANES else x


def far_groups(levels, planes):
    return -(-planes // (LANES // levels[3].win[2]))


def pack_far(levels, far_ref, planes):
    width = levels[3].win[2]
    per = LANES // width
    for group in range(far_ref.shape[0]):
        members = planes[per * group : per * group + per]
        far_ref[group] = total([turned(x, width * k) for k, x in enumerate(members)])


def unpack_far(levels, far_ref, at):
    width = levels[3].win[2]
    per = LANES // width
    return turned(far_ref[at // per], LANES - width * (at % per))


def lane_masks(levels):
    lane = lax.broadcasted_iota(jnp.int32, (8, LANES), 1)
    masks = []
    for level in levels[1:]:
        at = (lane + (2 * LANES - level.lane - REACH)) % LANES
        masks.append((at < level.win[2])[:1])
    return masks


def rows_kernel(levels, q_ref, prev_ref, next_ref, far_prev_ref, *refs):
    far_next_ref = far_prev_ref if len(refs) == 4 else refs[0]
    x_ref, up_ref, down_ref, far_ref = refs[-4:]
    count, pitch, rest_rows = slab_planes(levels), slab_pitch(levels), levels[2].rows
    masks = lane_masks(levels)
    coarsest = []

    def received(ref, at, level):
        slab = ref[at * pitch : (at + 1) * pitch].astype(F32)
        high = slab[: level.rows]
        return high if level.index == 1 else high + slab[rest_rows : rest_rows + level.rows]

    blocks = {True: {}, False: {}}
    for at in range(levels[1].full[0]):
        for level, mask in zip(levels[1:], masks):
            if at >= level.full[0]:
                continue
            n = level.n[0]
            terms = []
            if 0 <= at - REACH < level.win[0]:
                terms.append(q_ref[plane_at(levels, level, at - REACH, "own")])
            if at < count and at - REACH + n < level.win[0]:
                terms.append(received(prev_ref, at, level))
            if 0 <= at - REACH - n < count:
                terms.append(received(next_ref, at - REACH - n, level))
            if level.index == 3:
                if at - REACH + 2 * n < level.win[0]:
                    terms.append(unpack_far(levels, far_prev_ref, at - REACH + 2 * n))
                if at - REACH - 2 * n >= 0:
                    terms.append(unpack_far(levels, far_next_ref, at - REACH - 2 * n))
            value = jnp.where(mask, total(terms), 0.0)
            x_ref[plane_at(levels, level, at, "full")] = value
            first = level.n[1] - REACH
            for is_up, rows in ((True, value[first : first + SLAB]), (False, value[:SLAB])):
                high, rest = halves_of(rows)
                blocks[is_up].setdefault(at, []).append(high)
                if level.index > 1:
                    block, lanes = rest_block(levels, at)
                    blocks[is_up].setdefault(block, []).append(turned(rest, lanes))
            if level.index == 3:
                coarsest.append(value)
    for is_up, slab_ref in ((True, up_ref), (False, down_ref)):
        for block, parts in blocks[is_up].items():
            slab_ref[block * SLAB : (block + 1) * SLAB] = total(parts).astype(BF16)
    pack_far(levels, far_ref, coarsest)


def lanes_kernel(levels, table, x_ref, prev_ref, next_ref, far_prev_ref, *refs):
    far_next_ref = far_prev_ref if len(refs) == 8 else refs[0]
    table_ref, flat_refs, slab_refs, packed_refs = refs[-8], refs[-7:-5], refs[-5:-3], refs[-3:]

    def block_of(ref, block):
        return ref[block * SLAB : (block + 1) * SLAB].astype(F32)

    def received(ref, at, level):
        high = block_of(ref, at)
        if level.index == 1:
            return high
        block, lanes = rest_block(levels, at)
        return high + turned(block_of(ref, block), LANES - lanes)

    for level, mask in zip(levels[1:], lane_masks(levels)):
        blocks, step = level.inp[1] // 8, level.n[1] // 8
        flat_ref, packed_ref = flat_refs[level.index > 1], packed_refs[level.index - 1]
        for at in range(level.full[0]):
            own = x_ref[plane_at(levels, level, at, "full")]
            slabs = [received(prev_ref, at, level), received(next_ref, at, level)]
            if level.index == 3:
                slabs += [unpack_far(levels, ref, at) for ref in (far_prev_ref, far_next_ref)]
            parts = []
            for block in range(blocks):
                terms = []
                if 0 <= block - 1 < level.rows // 8:
                    terms.append(own[8 * block - 8 : 8 * block])
                places = [block, block - 1 - step, block - 1 + 2 * step, block - 1 - 2 * step]
                for slab, place in zip(slabs, places):
                    if 0 <= place < SLAB // 8:
                        terms.append(slab[8 * place : 8 * place + 8])
                parts.append(total(terms) if terms else jnp.zeros((8, LANES), F32))
            value = jnp.where(mask, jnp.concatenate(parts, 0), 0.0)
            first = level.flat + at * level.inp[1]
            flat_ref[first : first + level.inp[1]] = value
            sent = level.sent_rows
            packed_ref[at * sent : (at + 1) * sent] = value[:sent]
        used = level.full[0] * level.sent_rows
        if used < level.span:
            packed_ref[used:] = jnp.zeros((level.span - used, LANES), F32)
    shift = levels[2].span + levels[3].span
    for level, packed_ref in zip(levels[1:], packed_refs):
        slab_ref = slab_refs[level.index > 1]
        send = table.get(table_ref, "send", level.index)
        for first in range(0, level.span, 512):
            stop = min(first + 512, level.span)
            high, rest = halves_of(packed_ref[first:stop])
            where = slice(level.start + first, level.start + stop)
            slab_ref[:, where] = dot(send, high.astype(BF16), ((1,), (1,))).astype(BF16)
            if level.index > 1:
                where = slice(where.start + shift, where.stop + shift)
                slab_ref[:, where] = dot(send, rest.astype(BF16), ((1,), (1,))).astype(BF16)


def halo_kernel(wide_ref, out_ref):
    planes, rows, count = wide_ref.shape
    row = lax.broadcasted_iota(jnp.int32, (2 * REACH, count), 0)
    lane = lax.broadcasted_iota(jnp.int32, (2 * REACH, count), 1)
    send = jnp.where(lane == (row + (count - REACH)) % count, 1.0, 0.0).astype(BF16)
    step = 8
    for first in range(0, planes, step):
        chunk = wide_ref[first : first + step].reshape(step * rows, LANES)
        out_ref[:, first * rows : (first + step) * rows] = dot(send, chunk, ((1,), (1,))).astype(BF16)


def two_passes(level, band, first_ref, second_ref, put):
    def parts_of(result):
        parts = [result[:, :LANES], result[:, LANES:]]
        return jnp.concatenate([x.reshape(TILE, 8, LANES) for x in parts], 1)

    def along_y(pair):
        for block in range(level.out[1] // TILE):
            for term in range(4):
                halves = [
                    first_ref[
                        slice(pair * 16 + 8 * half, pair * 16 + 8 * half + 8),
                        TILE * block : TILE * block + 32,
                        term_lanes(term),
                    ].reshape(256, LANES)
                    for half in range(2)
                ]
                result = dot(band(term), jnp.concatenate(halves, 1))
                second_ref[
                    term, TILE * block : TILE * (block + 1), slice(pair * 16, pair * 16 + 16)
                ] = parts_of(result).astype(BF16)

    def along_x(pair):
        for block in range(level.out[0] // TILE):
            result = None
            for term in range(4):
                halves = [
                    second_ref[
                        term, slice(pair * 16 + 8 * half, pair * 16 + 8 * half + 8), TILE * block : TILE * block + 32
                    ].reshape(256, LANES)
                    for half in range(2)
                ]
                part = dot(band(term), jnp.concatenate(halves, 1))
                result = part if result is None else result + part
            put(block, pair, parts_of(result))

    for pair in range(level.inp[0] // 16):
        along_y(pair)
    for pair in range(level.out[1] // 16):
        along_x(pair)


def fine_kernel(level, wide_ref, halo_ref, lanes_ref, band_ref, out_ref, first_ref, second_ref):
    rows, step = level.inp[1], 16
    row = lax.broadcasted_iota(jnp.int32, (2 * REACH, LANES), 0)
    lane = lax.broadcasted_iota(jnp.int32, (2 * REACH, LANES), 1)
    place = jnp.where(lane == row, 1.0, 0.0).astype(BF16)

    @pl.loop(0, level.inp[0] // step)
    def _(chunk):
        where = pl.ds(pl.multiple_of(chunk * step * rows, LANES), step * rows)
        sides = dot(halo_ref[:, where], place, ((0,), (0,))).astype(BF16)
        here = wide_ref[pl.ds(chunk * step, step)].reshape(step * rows, LANES)
        result = dot(jnp.concatenate([here, sides], 1), lanes_ref[: 2 * LANES])
        first_ref[pl.ds(chunk * step, step)] = result.astype(BF16).reshape(step, rows, 4 * LANES)

    def put(block, pair, value):
        out_ref[TILE * block : TILE * (block + 1), slice(pair * 16, pair * 16 + 16)] = value

    two_passes(level, lambda term: band_ref[term], first_ref, second_ref, put)


def level_passes(levels, level, table, flat_ref, slab_ref, lanes_ref, band_ref, table_ref, first_ref, second_ref, sum_ref):
    shift = levels[2].span + levels[3].span
    rows, sent, step = level.inp[1], level.sent_rows, 16
    first_lane, _ = lane_rows(level)
    place = table.get(table_ref, "place", level.index)
    for plane in range(0, level.full[0], step):
        count = min(step, level.full[0] - plane)
        start = level.start + plane * sent
        stop = start + up_to(count * sent, LANES)
        slab = slab_ref[:, start:stop]
        if level.index > 1:
            slab = jnp.concatenate([slab, slab_ref[:, start + shift : stop + shift]], 0)
        extra = dot(slab, place, ((0,), (0,)))[: count * sent].reshape(count, sent, LANES)
        if sent < rows:
            extra = jnp.concatenate([extra, jnp.zeros((count, rows - sent, LANES), F32)], 1)
        first = level.flat + plane * rows
        value = flat_ref[first : first + count * rows] + extra.reshape(count * rows, LANES)
        result = dot(value.astype(BF16), lanes_ref[first_lane : first_lane + LANES])
        first_ref[plane : plane + count] = result.astype(BF16).reshape(count, rows, 4 * LANES)
    rest = level.inp[0] - plane - count
    if rest > 0:
        first_ref[plane + count :] = jnp.zeros((rest, rows, 4 * LANES), BF16)

    def put(block, pair, value):
        sum_ref[TILE * block : TILE * (block + 1), slice(pair * 16, pair * 16 + 16)] = value

    base = 4 * level.index
    two_passes(level, lambda term: band_ref[base + term], first_ref, second_ref, put)


def middle_kernel(levels, table, flat_ref, slab_ref, lanes_ref, band_ref, table_ref, sum_ref, first_ref, second_ref):
    level_passes(levels, levels[1], table, flat_ref, slab_ref, lanes_ref, band_ref, table_ref, first_ref, second_ref, sum_ref)


def coarse_kernel(levels, table, flat_ref, slab_ref, lanes_ref, band_ref, table_ref, middle_ref, fine_ref, *refs):
    out_hbm, first_refs, second_refs, sum_refs, out_ref, sems = refs[0], refs[1:3], refs[3:5], refs[5:8], refs[8], refs[9]
    for level in (levels[3], levels[2]):
        which = level.index - 2
        level_passes(
            levels, level, table, flat_ref, slab_ref, lanes_ref, band_ref, table_ref,
            first_refs[which], second_refs[which], sum_refs[level.index - 1],
        )

    def stretch(fine, coarse, source):
        planes, rows, _ = source.shape
        for first in range(0, coarse.win[0], 4):
            count = min(4, planes - first)
            value = split_lanes(source[first : first + count].reshape(count * rows, LANES))
            value = dot(value, table.get(table_ref, "zed", fine.index))
            source[first : first + count] = value.reshape(count, rows, LANES)

    def prolong(fine, coarse, halves, source, emit):
        planes = []
        for half in halves:
            at = half + coarse.low
            between = (9.0 * (source[at] + source[at + 1]) - (source[at - 1] + source[at + 2])) / 16.0
            planes += [split_rows(source[at]), split_rows(between)]
        both = dot(table.get(table_ref, "tall", fine.index), jnp.concatenate(planes, 1))
        for k, half in enumerate(halves):
            emit(2 * half, both[:, 2 * k * LANES : (2 * k + 1) * LANES])
            emit(2 * half + 1, both[:, (2 * k + 1) * LANES : (2 * k + 2) * LANES])

    for fine, coarse in ((levels[2], levels[3]), (levels[1], levels[2])):
        sum_ref = sum_refs[fine.index - 1]
        source = sum_refs[coarse.index - 1]
        stretch(fine, coarse, source)

        def emit(at, value, fine=fine, sum_ref=sum_ref):
            plane = at + fine.low
            if 0 <= plane < fine.win[0]:
                sum_ref[plane] = (middle_ref if fine.index == 1 else sum_ref)[plane] + value

        for half in range(-1, (fine.n[0] + fine.high + 1) // 2):
            prolong(fine, coarse, [half], source, emit)

    stretch(levels[0], levels[1], sum_refs[0])

    def emit_fine(at, value):
        out_ref[at] = (fine_ref[at] + value).astype(BF16)

    copies = []
    for group in range(levels[0].n[0] // 8):
        prolong(levels[0], levels[1], [4 * group + k for k in range(4)], sum_refs[0], emit_fine)
        where = slice(8 * group, 8 * group + 8)
        copies.append(pltpu.make_async_copy(out_ref.at[where], out_hbm.at[where], sems.at[group]))
        copies[-1].start()
    for copy in copies:
        copy.wait()


def make_table(levels):
    table = Table()
    for level, fine in zip(levels[1:], levels[:3]):
        table.add(("send", level.index), send_lanes(level))
        table.add(("place", level.index), place_lanes(level))
        table.add(("tall", fine.index), prolong_rows(fine, level))
        table.add(("zed", fine.index), prolong_lanes(fine, level))
    return table


def ends_kernel(charges_ref, last_ref, first_ref):
    last_ref[...] = charges_ref[charges_ref.shape[0] - REACH :]
    first_ref[...] = charges_ref[:REACH]


def call(kernel, out_shape, args, scratch=(), spaces={}, out_space=pltpu.VMEM, flops=0, limit=12):
    specs = [pl.BlockSpec(memory_space=spaces.get(i, pltpu.VMEM)) for i in range(len(args))]
    single = not isinstance(out_shape, (list, tuple))
    outs = [out_shape] if single else list(out_shape)
    out_specs = [pl.BlockSpec(memory_space=out_space) for _ in outs]
    return pl.pallas_call(
        kernel,
        out_shape=out_shape,
        in_specs=specs,
        out_specs=out_specs[0] if single else out_specs,
        scratch_shapes=list(scratch),
        compiler_params=pltpu.CompilerParams(vmem_limit_bytes=limit << 20),
        cost_estimate=pl.CostEstimate(flops=flops, bytes_accessed=1 << 20, transcendentals=0),
    )(*args)


def shape(sizes, dtype):
    return jax.ShapeDtypeStruct(tuple(sizes), dtype)


def shifted(value, axis, by):
    count = lax.axis_size(axis)
    return lax.ppermute(value, axis, [(i, (i + by) % count) for i in range(count)])


def far_pair(value, axis):
    after = shifted(value, axis, 2)
    return [after] if lax.axis_size(axis) == 4 else [after, shifted(value, axis, -2)]


def z_pair(value, axis):
    half = value.shape[0] // 2
    if lax.axis_size(axis) == 2:
        return shifted(value, axis, 1)
    return jnp.concatenate([shifted(value[:half], axis, 1), shifted(value[half:], axis, -1)], 0)


def steps(charges, taps):
    levels = levels_of(charges.shape)
    table = make_table(levels)
    table_array = table.array()
    zero, coarse = levels[0], levels[1:]
    reach = REACH

    last, first = call(
        ends_kernel, [shape((reach, *charges.shape[1:]), BF16)] * 2, [charges], flops=1 << 20
    )
    x_prev = shifted(last, "gx", 1)
    x_next = shifted(first, "gx", -1)

    x_slab = shape((slab_planes(levels) * slab_pitch(levels), LANES), BF16)
    q, up, down, far = call(
        functools.partial(restrict_kernel, levels),
        [
            shape((sum(lv.win[0] * lv.rows for lv in coarse), LANES), F32),
            x_slab,
            x_slab,
            shape((far_groups(levels, levels[3].win[0]), SLAB, LANES), F32),
        ],
        [charges],
        flops=1 << 27,
    )
    band, lanes = call(
        functools.partial(bands_kernel, levels),
        [shape((16, 8 * TILE, 16 * TILE), BF16), shape((5 * LANES, 4 * LANES), BF16)],
        [taps.reshape(16, 17)],
        spaces={0: pltpu.SMEM},
        flops=1 << 26,
    )
    from_prev = shifted(up, "gx", 1)
    from_next = shifted(down, "gx", -1)
    far = far_pair(far, "gx")
    pieces = (x_prev, charges, x_next)
    y_prev = shifted(jnp.concatenate([x[:, -reach:] for x in pieces], 0), "gy", 1)
    y_next = shifted(jnp.concatenate([x[:, :reach] for x in pieces], 0), "gy", -1)

    y_slab = shape((slab_blocks(levels) * SLAB, LANES), BF16)
    r, up, down, far = call(
        functools.partial(rows_kernel, levels),
        [
            shape((sum(lv.full[0] * lv.rows for lv in coarse), LANES), F32),
            y_slab,
            y_slab,
            shape((far_groups(levels, levels[3].full[0]), SLAB, LANES), F32),
        ],
        [q, from_prev, from_next, *far],
        flops=1 << 25,
    )
    m_prev = shifted(up, "gy", 1)
    m_next = shifted(down, "gy", -1)
    far = far_pair(far, "gy")

    wide = jnp.concatenate([y_prev, jnp.concatenate(pieces, 0), y_next], 1)
    sides = call(
        halo_kernel,
        shape((2 * reach, wide.shape[0] * wide.shape[1]), BF16),
        [wide],
        flops=1 << 26,
    )
    halo = z_pair(sides, "gz")

    flat_rows = [lv.full[0] * lv.inp[1] for lv in coarse]
    slab_shapes = [
        (2 * coarse[0].sent, coarse[0].span),
        (2 * coarse[1].sent, 2 * (coarse[1].span + coarse[2].span)),
    ]
    *flats, slab_one, slab_two = call(
        functools.partial(lanes_kernel, levels, table),
        [shape((count, LANES), F32) for count in (flat_rows[0], flat_rows[1] + flat_rows[2])]
        + [shape(sizes, BF16) for sizes in slab_shapes],
        [r, m_prev, m_next, *far, table_array],
        scratch=[pltpu.VMEM((lv.span, LANES), F32) for lv in coarse],
        flops=1 << 26,
    )
    slab_one = z_pair(slab_one, "gz")
    slab_two = z_pair(slab_two, "gz")

    fine = call(
        functools.partial(fine_kernel, zero),
        shape(charges.shape, F32),
        [wide, halo, lanes, band],
        scratch=[
            pltpu.VMEM((*zero.inp, 4 * LANES), BF16),
            pltpu.VMEM((4, zero.out[1], zero.inp[0], LANES), BF16),
        ],
        flops=1 << 32,
        limit=20,
    )
    slab_one, fine = lax.optimization_barrier((slab_one, fine))

    def scratch(some):
        return [pltpu.VMEM((*lv.inp, 4 * LANES), BF16) for lv in some] + [
            pltpu.VMEM((4, lv.out[1], lv.inp[0], LANES), BF16) for lv in some
        ]

    middle = call(
        functools.partial(middle_kernel, levels, table),
        shape((*coarse[0].out, LANES), F32),
        [flats[0], slab_one, lanes, band, table_array],
        scratch=scratch(coarse[:1]),
        flops=1 << 31,
        limit=16,
    )
    return call(
        functools.partial(coarse_kernel, levels, table),
        shape(charges.shape, BF16),
        [flats[1], slab_two, lanes, band, table_array, middle, fine],
        scratch=scratch(coarse[1:])
        + [pltpu.VMEM((*lv.out, LANES), F32) for lv in coarse]
        + [pltpu.VMEM(charges.shape, BF16), pltpu.SemaphoreType.DMA((charges.shape[0] // 8,))],
        out_space=pl.ANY,
        flops=1 << 30,
        limit=16,
    )


def solution(mesh):
    return jax.shard_map(
        steps,
        mesh=mesh,
        in_specs=(P("gx", "gy", "gz"), P()),
        out_specs=P("gx", "gy", "gz"),
        check_vma=False,
    )
```

```python
import functools

import jax
import jax.numpy as jnp
import numpy as np
from jax import lax
from jax.experimental import pallas as pl
from jax.experimental.pallas import tpu as pltpu
from jax.sharding import PartitionSpec as P


F32, BF16 = jnp.float32, jnp.bfloat16
REACH = 8
LANES = 128
TILE = 16
SLAB = 16
LOW, HIGH = (0, 1, 2, 2), (0, 2, 3, 3)
STENCIL = ((0, 1.0), (-1, 9 / 16), (1, 9 / 16), (-3, -1 / 16), (3, -1 / 16))


def up_to(value, step):
    return -(-value // step) * step


class Level:
    def __init__(self, index, block):
        self.index = index
        self.n = tuple(size >> index for size in block)
        self.low, self.high = LOW[index], HIGH[index]
        self.win = tuple(size + self.low + self.high for size in self.n)
        self.full = tuple(size + 2 * REACH for size in self.win)
        self.out = tuple(up_to(size, TILE) for size in self.win[:2])
        self.inp = tuple(size + TILE for size in self.out)
        self.rows = up_to(self.win[1], 8)
        self.lane = 0
        self.start = self.flat = 0
        self.sent_rows = up_to(self.full[1], 8)
        self.span = up_to(self.full[0] * self.sent_rows, LANES)
        self.sent = up_to(self.low + self.high + REACH, 4)


def levels_of(block):
    levels = [Level(index, block) for index in range(4)]
    lane = 0
    for level in levels[1:]:
        level.lane = lane
        lane += level.win[2]
    levels[3].start = levels[2].span
    levels[3].flat = levels[2].full[0] * levels[2].inp[1]
    assert lane <= LANES and block[2] == LANES
    assert all(level.n[d] % 8 == 0 for level in levels for d in range(3))
    return levels


def own_lane(level, z):
    return (level.lane + z + level.low + REACH) % LANES


def stencil_of(offset, valid):
    size = jnp.abs(offset)
    weight = jnp.where(size == 0, 1.0, jnp.where(size == 1, 9 / 16, jnp.where(size == 3, -1 / 16, 0.0)))
    return jnp.where(valid, weight, 0.0).astype(BF16)


def restrict_rows(coarse, fine):
    fine_rows = fine.n[1] if fine.index == 0 else fine.rows
    row = lax.broadcasted_iota(jnp.int32, (coarse.rows, 2 * fine_rows), 0)
    col = lax.broadcasted_iota(jnp.int32, (coarse.rows, 2 * fine_rows), 1)
    col = jnp.where(col >= fine_rows, col - fine_rows, col)
    valid = (row < coarse.win[1]) & (col < fine.win[1])
    return stencil_of(col - fine.low - 2 * (row - coarse.low), valid)


def restrict_lanes(coarse, fine):
    k = lax.broadcasted_iota(jnp.int32, (2 * LANES, LANES), 0) % LANES
    lane = lax.broadcasted_iota(jnp.int32, (2 * LANES, LANES), 1)

    def place(level, lanes):
        return lanes if level.index == 0 else (lanes + (2 * LANES - level.lane - REACH)) % LANES

    k, lane = place(fine, k), place(coarse, lane)
    valid = (k < fine.win[2]) & (lane < coarse.win[2])
    return stencil_of(k - fine.low - 2 * (lane - coarse.low), valid)


def prolong_weights(fine_at):
    half = fine_at // 2
    if fine_at % 2 == 0:
        return ((half, 1.0),)
    return ((half, 9 / 16), (half + 1, 9 / 16), (half - 1, -1 / 16), (half + 2, -1 / 16))


def prolong_matrix(fine_count, fine_win, fine_low, coarse_count, coarse_low):
    matrix = np.zeros((fine_count, coarse_count))
    for row in range(fine_win):
        for at, weight in prolong_weights(row - fine_low):
            if 0 <= at + coarse_low < coarse_count:
                matrix[row, at + coarse_low] = weight
    return matrix


def prolong_rows(fine, coarse):
    matrix = prolong_matrix(fine.out[1], fine.win[1], fine.low, coarse.out[1], coarse.low)
    return np.concatenate([matrix, matrix], 1)


def prolong_lanes(fine, coarse):
    matrix = prolong_matrix(LANES, fine.win[2], fine.low, LANES, coarse.low).T
    return np.concatenate([matrix, matrix], 0)


def send_lanes(level):
    up, down = np.zeros((level.sent, LANES)), np.zeros((level.sent, LANES))
    for j in range(level.sent):
        s = level.n[2] - REACH + j
        if s < level.win[2]:
            up[j, own_lane(level, s - level.low)] = 1
        if j < level.low + level.high + REACH:
            down[j, own_lane(level, j - level.low)] = 1
    return np.concatenate([up, down], 0)


def place_lanes(level):
    from_prev, from_next = np.zeros((level.sent, LANES)), np.zeros((level.sent, LANES))
    for j in range(level.sent):
        if level.n[2] - REACH + j < level.win[2]:
            from_prev[j, (level.lane + j) % LANES] = 1
        at = j + REACH + level.n[2]
        if at < level.full[2]:
            from_next[j, (level.lane + at) % LANES] = 1
    return np.concatenate([from_prev, from_next] * (1 if level.index == 1 else 2), 0)


def dot(a, b, dims=((1,), (0,))):
    return lax.dot_general(a, b, (dims, ((), ())), preferred_element_type=F32)


def split_rows(x):
    high = x.astype(BF16).astype(F32)
    return jnp.concatenate([high, x - high], 0).astype(BF16)


def split_lanes(x):
    high = x.astype(BF16).astype(F32)
    return jnp.concatenate([high, x - high], 1).astype(BF16)


class Table:
    def __init__(self):
        self.parts, self.places, self.count = [], {}, 0

    def add(self, key, matrix):
        rows, cols = matrix.shape
        padded = np.zeros((up_to(rows, TILE), LANES), np.float32)
        padded[:rows, :cols] = matrix
        self.places[key] = (self.count, rows, cols)
        self.parts.append(padded)
        self.count += padded.shape[0]

    def array(self):
        return jnp.asarray(np.concatenate(self.parts, 0), BF16)

    def get(self, ref, *key):
        start, rows, cols = self.places[key]
        return ref[start : start + rows, :cols]


def pad_rows(x, rows):
    if x.shape[0] == rows:
        return x
    return jnp.concatenate([x, jnp.zeros((rows - x.shape[0], x.shape[1]), x.dtype)], 0)


def total(terms):
    return functools.reduce(lambda a, b: a + b, terms)


def bands_kernel(levels, taps_ref, band_ref, lanes_ref):
    row = lax.broadcasted_iota(jnp.int32, (8 * TILE, 16 * TILE), 0)
    col = lax.broadcasted_iota(jnp.int32, (8 * TILE, 16 * TILE), 1)
    offset = jnp.where(row % 8 == col // 32, col % 32 - row // 8, -1)

    @pl.loop(0, 16)
    def _(which):
        matrix = jnp.zeros(offset.shape, F32)
        for tap in range(17):
            matrix = jnp.where(offset == tap, taps_ref[which, tap], matrix)
        band_ref[which] = matrix.astype(BF16)

    for level in levels:
        first, count = lane_rows(level)
        k = lax.broadcasted_iota(jnp.int32, (count, LANES), 0)
        z_out = lax.broadcasted_iota(jnp.int32, (count, LANES), 1)
        if level.index == 0:
            n = level.n[2]
            z_in = jnp.where(k < n, k + REACH, jnp.where(k < n + REACH, k - n, k))
            valid = k < n + 2 * REACH
        else:
            z_in = (k + (LANES - level.lane)) % LANES
            valid = (z_in < level.full[2]) & (z_out < level.win[2])
        offset_z = jnp.where(valid, z_in - z_out, -1)
        for term in range(4):
            matrix = jnp.zeros(offset_z.shape, F32)
            for tap in range(17):
                matrix = jnp.where(offset_z == tap, taps_ref[4 * level.index + term, tap], matrix)
            lanes_ref[first : first + count, term_lanes(term)] = matrix.astype(BF16)


def lane_rows(level):
    return (0, 2 * LANES) if level.index == 0 else ((level.index + 1) * LANES, LANES)


def term_lanes(term):
    return slice(term * LANES, (term + 1) * LANES)


def plane_at(levels, level, which, rows):
    first = 0
    for other in levels[1:]:
        sizes = (other.win[0], other.rows) if rows == "own" else (other.full[0], other.rows)
        if other is level:
            return slice(first + which * sizes[1], first + (which + 1) * sizes[1])
        first += sizes[0] * sizes[1]
    return first


def halves_of(x):
    high = x.astype(BF16).astype(F32)
    return high, x - high


def restrict_kernel(
    levels, charges_ref, q_ref, up_ref, down_ref, far_ref
):
    for level, fine in zip(levels[1:], levels[:3]):
        by_rows, by_lanes = restrict_rows(level, fine), restrict_lanes(level, fine)
        for at in range(level.win[0]):
            terms = {}
            for offset, weight in STENCIL:
                plane = 2 * (at - level.low) + offset + fine.low
                if 0 <= plane < fine.win[0]:
                    if fine.index == 0:
                        value = charges_ref[plane].astype(F32)
                    else:
                        value = q_ref[plane_at(levels, fine, plane, "own")]
                    terms.setdefault(weight, []).append(value)
            value = total([total(group) * weight for weight, group in terms.items()])
            value = dot(by_rows, split_rows(value))
            value = dot(split_lanes(value), by_lanes)
            q_ref[plane_at(levels, level, at, "own")] = value
    high_rows, rest_rows = levels[1].rows, levels[2].rows
    pitch = slab_pitch(levels)
    planes = slab_planes(levels)
    for j in range(planes):
        for slab_ref, bases in ((up_ref, [lv.n[0] - REACH for lv in levels[1:]]), (down_ref, [0] * 3)):
            highs, rests = [], [jnp.zeros((rest_rows, LANES), F32)]
            for level, base in zip(levels[1:], bases):
                if base + j < level.win[0]:
                    high, rest = halves_of(q_ref[plane_at(levels, level, base + j, "own")])
                    highs.append(pad_rows(high, high_rows))
                    if level.index > 1:
                        rests.append(pad_rows(rest, rest_rows))
            rest = jnp.concatenate([jnp.zeros((rest_rows, LANES), F32), total(rests)], 0)
            value = pad_rows(total(highs), pitch) + rest
            slab_ref[j * pitch : (j + 1) * pitch] = value.astype(BF16)
    last = levels[3]
    pack_far(
        levels,
        far_ref,
        [q_ref[plane_at(levels, last, at, "own")] for at in range(last.win[0])],
    )


def slab_planes(levels):
    return max(level.low + level.high + REACH for level in levels[1:])


def slab_pitch(levels):
    return up_to(max(levels[1].rows, 2 * levels[2].rows), TILE)


def rest_block(levels, plane):
    spare = levels[1].full[0] - levels[2].full[0]
    if plane < spare:
        return levels[2].full[0] + plane, 0
    return levels[1].full[0] + (plane - spare) // 2, LANES // 2 * ((plane - spare) % 2)


def slab_blocks(levels):
    return rest_block(levels, levels[2].full[0] - 1)[0] + 1


def turned(x, lanes):
    return pltpu.roll(x, lanes % LANES, 1) if lanes % LANES else x


def far_groups(levels, planes):
    return -(-planes // (LANES // levels[3].win[2]))


def pack_far(levels, far_ref, planes):
    width = levels[3].win[2]
    per = LANES // width
    for group in range(far_ref.shape[0]):
        members = planes[per * group : per * group + per]
        far_ref[group] = total([turned(x, width * k) for k, x in enumerate(members)])


def unpack_far(levels, far_ref, at):
    width = levels[3].win[2]
    per = LANES // width
    return turned(far_ref[at // per], LANES - width * (at % per))


def lane_masks(levels):
    lane = lax.broadcasted_iota(jnp.int32, (8, LANES), 1)
    masks = []
    for level in levels[1:]:
        at = (lane + (2 * LANES - level.lane - REACH)) % LANES
        masks.append((at < level.win[2])[:1])
    return masks


def rows_kernel(levels, q_ref, prev_ref, next_ref, far_prev_ref, *refs):
    far_next_ref = far_prev_ref if len(refs) == 4 else refs[0]
    x_ref, up_ref, down_ref, far_ref = refs[-4:]
    count, pitch, rest_rows = slab_planes(levels), slab_pitch(levels), levels[2].rows
    masks = lane_masks(levels)
    coarsest = []

    def received(ref, at, level):
        slab = ref[at * pitch : (at + 1) * pitch].astype(F32)
        high = slab[: level.rows]
        return high if level.index == 1 else high + slab[rest_rows : rest_rows + level.rows]

    blocks = {True: {}, False: {}}
    for at in range(levels[1].full[0]):
        for level, mask in zip(levels[1:], masks):
            if at >= level.full[0]:
                continue
            n = level.n[0]
            terms = []
            if 0 <= at - REACH < level.win[0]:
                terms.append(q_ref[plane_at(levels, level, at - REACH, "own")])
            if at < count and at - REACH + n < level.win[0]:
                terms.append(received(prev_ref, at, level))
            if 0 <= at - REACH - n < count:
                terms.append(received(next_ref, at - REACH - n, level))
            if level.index == 3:
                if at - REACH + 2 * n < level.win[0]:
                    terms.append(unpack_far(levels, far_prev_ref, at - REACH + 2 * n))
                if at - REACH - 2 * n >= 0:
                    terms.append(unpack_far(levels, far_next_ref, at - REACH - 2 * n))
            value = jnp.where(mask, total(terms), 0.0)
            x_ref[plane_at(levels, level, at, "full")] = value
            first = level.n[1] - REACH
            for is_up, rows in ((True, value[first : first + SLAB]), (False, value[:SLAB])):
                high, rest = halves_of(rows)
                blocks[is_up].setdefault(at, []).append(high)
                if level.index > 1:
                    block, lanes = rest_block(levels, at)
                    blocks[is_up].setdefault(block, []).append(turned(rest, lanes))
            if level.index == 3:
                coarsest.append(value)
    for is_up, slab_ref in ((True, up_ref), (False, down_ref)):
        for block, parts in blocks[is_up].items():
            slab_ref[block * SLAB : (block + 1) * SLAB] = total(parts).astype(BF16)
    pack_far(levels, far_ref, coarsest)


def lanes_kernel(levels, some, table, x_ref, prev_ref, next_ref, table_ref, *refs):
    far_refs, (flat_ref, slab_ref) = refs[: -2 - len(some)], refs[-2 - len(some) : -len(some)]
    packed_refs = refs[-len(some) :]
    masks = dict(zip(range(1, 4), lane_masks(levels)))

    def block_of(ref, block):
        return ref[block * SLAB : (block + 1) * SLAB].astype(F32)

    def received(ref, at, level):
        high = block_of(ref, at)
        if level.index == 1:
            return high
        block, lanes = rest_block(levels, at)
        return high + turned(block_of(ref, block), LANES - lanes)

    for level, packed_ref in zip(some, packed_refs):
        mask = masks[level.index]
        blocks, step = level.inp[1] // 8, level.n[1] // 8
        for at in range(level.full[0]):
            own = x_ref[plane_at(levels, level, at, "full")]
            slabs = [received(prev_ref, at, level), received(next_ref, at, level)]
            if level.index == 3:
                slabs += [unpack_far(levels, ref, at) for ref in (far_refs[0], far_refs[-1])]
            parts = []
            for block in range(blocks):
                terms = []
                if 0 <= block - 1 < level.rows // 8:
                    terms.append(own[8 * block - 8 : 8 * block])
                places = [block, block - 1 - step, block - 1 + 2 * step, block - 1 - 2 * step]
                for slab, place in zip(slabs, places):
                    if 0 <= place < SLAB // 8:
                        terms.append(slab[8 * place : 8 * place + 8])
                parts.append(total(terms) if terms else jnp.zeros((8, LANES), F32))
            value = jnp.where(mask, jnp.concatenate(parts, 0), 0.0)
            first = level.flat + at * level.inp[1]
            flat_ref[first : first + level.inp[1]] = value
            sent = level.sent_rows
            packed_ref[at * sent : (at + 1) * sent] = value[:sent]
        used = level.full[0] * level.sent_rows
        if used < level.span:
            packed_ref[used:] = jnp.zeros((level.span - used, LANES), F32)
    shift = levels[2].span + levels[3].span
    for level, packed_ref in zip(some, packed_refs):
        send = table.get(table_ref, "send", level.index)
        for first in range(0, level.span, 512):
            stop = min(first + 512, level.span)
            high, rest = halves_of(packed_ref[first:stop])
            where = slice(level.start + first, level.start + stop)
            slab_ref[:, where] = dot(send, high.astype(BF16), ((1,), (1,))).astype(BF16)
            if level.index > 1:
                where = slice(where.start + shift, where.stop + shift)
                slab_ref[:, where] = dot(send, rest.astype(BF16), ((1,), (1,))).astype(BF16)


def halo_kernel(wide_ref, out_ref):
    planes, rows, count = wide_ref.shape
    row = lax.broadcasted_iota(jnp.int32, (2 * REACH, count), 0)
    lane = lax.broadcasted_iota(jnp.int32, (2 * REACH, count), 1)
    send = jnp.where(lane == (row + (count - REACH)) % count, 1.0, 0.0).astype(BF16)
    step = 8
    for first in range(0, planes, step):
        chunk = wide_ref[first : first + step].reshape(step * rows, LANES)
        out_ref[:, first * rows : (first + step) * rows] = dot(send, chunk, ((1,), (1,))).astype(BF16)


def two_passes(level, band, first_ref, second_ref, put):
    def parts_of(result):
        parts = [result[:, :LANES], result[:, LANES:]]
        return jnp.concatenate([x.reshape(TILE, 8, LANES) for x in parts], 1)

    def along_y(pair):
        for block in range(level.out[1] // TILE):
            for term in range(4):
                halves = [
                    first_ref[
                        slice(pair * 16 + 8 * half, pair * 16 + 8 * half + 8),
                        TILE * block : TILE * block + 32,
                        term_lanes(term),
                    ].reshape(256, LANES)
                    for half in range(2)
                ]
                result = dot(band(term), jnp.concatenate(halves, 1))
                second_ref[
                    term, TILE * block : TILE * (block + 1), slice(pair * 16, pair * 16 + 16)
                ] = parts_of(result).astype(BF16)

    def along_x(pair):
        for block in range(level.out[0] // TILE):
            result = None
            for term in range(4):
                halves = [
                    second_ref[
                        term, slice(pair * 16 + 8 * half, pair * 16 + 8 * half + 8), TILE * block : TILE * block + 32
                    ].reshape(256, LANES)
                    for half in range(2)
                ]
                part = dot(band(term), jnp.concatenate(halves, 1))
                result = part if result is None else result + part
            put(block, pair, parts_of(result))

    for pair in range(level.inp[0] // 16):
        along_y(pair)
    for pair in range(level.out[1] // 16):
        along_x(pair)


def fine_kernel(level, wide_ref, halo_ref, lanes_ref, band_ref, out_ref, first_ref, second_ref):
    rows, step = level.inp[1], 16
    row = lax.broadcasted_iota(jnp.int32, (2 * REACH, LANES), 0)
    lane = lax.broadcasted_iota(jnp.int32, (2 * REACH, LANES), 1)
    place = jnp.where(lane == row, 1.0, 0.0).astype(BF16)

    for chunk in range(level.inp[0] // step):
        where = slice(chunk * step * rows, (chunk + 1) * step * rows)
        sides = dot(halo_ref[:, where], place, ((0,), (0,))).astype(BF16)
        here = wide_ref[chunk * step : (chunk + 1) * step].reshape(step * rows, LANES)
        result = dot(jnp.concatenate([here, sides], 1), lanes_ref[: 2 * LANES])
        first_ref[chunk * step : (chunk + 1) * step] = result.astype(BF16).reshape(step, rows, 4 * LANES)

    def put(block, pair, value):
        out_ref[TILE * block : TILE * (block + 1), slice(pair * 16, pair * 16 + 16)] = value

    two_passes(level, lambda term: band_ref[term], first_ref, second_ref, put)


def level_passes(levels, level, table, flat_ref, slab_ref, lanes_ref, band_ref, table_ref, first_ref, second_ref, sum_ref):
    shift = levels[2].span + levels[3].span
    rows, sent, step = level.inp[1], level.sent_rows, 16
    first_lane, _ = lane_rows(level)
    place = table.get(table_ref, "place", level.index)
    for plane in range(0, level.full[0], step):
        count = min(step, level.full[0] - plane)
        start = level.start + plane * sent
        stop = start + up_to(count * sent, LANES)
        slab = slab_ref[:, start:stop]
        if level.index > 1:
            slab = jnp.concatenate([slab, slab_ref[:, start + shift : stop + shift]], 0)
        extra = dot(slab, place, ((0,), (0,)))[: count * sent].reshape(count, sent, LANES)
        if sent < rows:
            extra = jnp.concatenate([extra, jnp.zeros((count, rows - sent, LANES), F32)], 1)
        first = level.flat + plane * rows
        value = flat_ref[first : first + count * rows] + extra.reshape(count * rows, LANES)
        result = dot(value.astype(BF16), lanes_ref[first_lane : first_lane + LANES])
        first_ref[plane : plane + count] = result.astype(BF16).reshape(count, rows, 4 * LANES)
    rest = level.inp[0] - plane - count
    if rest > 0:
        first_ref[plane + count :] = jnp.zeros((rest, rows, 4 * LANES), BF16)

    def put(block, pair, value):
        sum_ref[TILE * block : TILE * (block + 1), slice(pair * 16, pair * 16 + 16)] = value

    base = 4 * level.index
    two_passes(level, lambda term: band_ref[base + term], first_ref, second_ref, put)


def middle_kernel(levels, table, flat_ref, slab_ref, lanes_ref, band_ref, table_ref, sum_ref, first_ref, second_ref):
    level_passes(levels, levels[1], table, flat_ref, slab_ref, lanes_ref, band_ref, table_ref, first_ref, second_ref, sum_ref)


def coarse_kernel(levels, table, flat_ref, slab_ref, lanes_ref, band_ref, table_ref, middle_ref, fine_ref, *refs):
    out_hbm, first_refs, second_refs, sum_refs, out_ref, sems = refs[0], refs[1:3], refs[3:5], refs[5:8], refs[8], refs[9]
    for level in (levels[3], levels[2]):
        which = level.index - 2
        level_passes(
            levels, level, table, flat_ref, slab_ref, lanes_ref, band_ref, table_ref,
            first_refs[which], second_refs[which], sum_refs[level.index - 1],
        )

    def stretch(fine, coarse, source):
        planes, rows, _ = source.shape
        for first in range(0, coarse.win[0], 4):
            count = min(4, planes - first)
            value = split_lanes(source[first : first + count].reshape(count * rows, LANES))
            value = dot(value, table.get(table_ref, "zed", fine.index))
            source[first : first + count] = value.reshape(count, rows, LANES)

    def prolong(fine, coarse, halves, source, emit):
        planes = []
        for half in halves:
            at = half + coarse.low
            between = (9.0 * (source[at] + source[at + 1]) - (source[at - 1] + source[at + 2])) / 16.0
            planes += [split_rows(source[at]), split_rows(between)]
        both = dot(table.get(table_ref, "tall", fine.index), jnp.concatenate(planes, 1))
        for k, half in enumerate(halves):
            emit(2 * half, both[:, 2 * k * LANES : (2 * k + 1) * LANES])
            emit(2 * half + 1, both[:, (2 * k + 1) * LANES : (2 * k + 2) * LANES])

    for fine, coarse in ((levels[2], levels[3]), (levels[1], levels[2])):
        sum_ref = sum_refs[fine.index - 1]
        source = sum_refs[coarse.index - 1]
        stretch(fine, coarse, source)

        def emit(at, value, fine=fine, sum_ref=sum_ref):
            plane = at + fine.low
            if 0 <= plane < fine.win[0]:
                sum_ref[plane] = (middle_ref if fine.index == 1 else sum_ref)[plane] + value

        for half in range(-1, (fine.n[0] + fine.high + 1) // 2):
            prolong(fine, coarse, [half], source, emit)

    stretch(levels[0], levels[1], sum_refs[0])

    def emit_fine(at, value):
        out_ref[at] = (fine_ref[at] + value).astype(BF16)

    copies = []
    for group in range(levels[0].n[0] // 8):
        prolong(levels[0], levels[1], [4 * group + k for k in range(4)], sum_refs[0], emit_fine)
        where = slice(8 * group, 8 * group + 8)
        copies.append(pltpu.make_async_copy(out_ref.at[where], out_hbm.at[where], sems.at[group]))
        copies[-1].start()
    for copy in copies:
        copy.wait()


def make_table(levels):
    table = Table()
    for level, fine in zip(levels[1:], levels[:3]):
        table.add(("send", level.index), send_lanes(level))
        table.add(("place", level.index), place_lanes(level))
        table.add(("tall", fine.index), prolong_rows(fine, level))
        table.add(("zed", fine.index), prolong_lanes(fine, level))
    return table


def ends_kernel(charges_ref, last_ref, first_ref):
    last_ref[...] = charges_ref[charges_ref.shape[0] - REACH :]
    first_ref[...] = charges_ref[:REACH]


def call(kernel, out_shape, args, scratch=(), spaces={}, out_space=pltpu.VMEM, flops=0, limit=12):
    specs = [pl.BlockSpec(memory_space=spaces.get(i, pltpu.VMEM)) for i in range(len(args))]
    single = not isinstance(out_shape, (list, tuple))
    outs = [out_shape] if single else list(out_shape)
    out_specs = [pl.BlockSpec(memory_space=out_space) for _ in outs]
    return pl.pallas_call(
        kernel,
        out_shape=out_shape,
        in_specs=specs,
        out_specs=out_specs[0] if single else out_specs,
        scratch_shapes=list(scratch),
        compiler_params=pltpu.CompilerParams(vmem_limit_bytes=limit << 20),
        cost_estimate=pl.CostEstimate(flops=flops, bytes_accessed=1 << 20, transcendentals=0),
    )(*args)


def shape(sizes, dtype):
    return jax.ShapeDtypeStruct(tuple(sizes), dtype)


def shifted(value, axis, by):
    count = lax.axis_size(axis)
    return lax.ppermute(value, axis, [(i, (i + by) % count) for i in range(count)])


def far_pair(value, axis):
    after = shifted(value, axis, 2)
    return [after] if lax.axis_size(axis) == 4 else [after, shifted(value, axis, -2)]


def z_pair(value, axis):
    half = value.shape[0] // 2
    if lax.axis_size(axis) == 2:
        return shifted(value, axis, 1)
    return jnp.concatenate([shifted(value[:half], axis, 1), shifted(value[half:], axis, -1)], 0)


def steps(charges, taps):
    levels = levels_of(charges.shape)
    table = make_table(levels)
    table_array = table.array()
    zero, coarse = levels[0], levels[1:]
    reach = REACH

    last, first = call(
        ends_kernel, [shape((reach, *charges.shape[1:]), BF16)] * 2, [charges], flops=1 << 20
    )
    x_prev = shifted(last, "gx", 1)
    x_next = shifted(first, "gx", -1)

    x_slab = shape((slab_planes(levels) * slab_pitch(levels), LANES), BF16)
    q, up, down, far = call(
        functools.partial(restrict_kernel, levels),
        [
            shape((sum(lv.win[0] * lv.rows for lv in coarse), LANES), F32),
            x_slab,
            x_slab,
            shape((far_groups(levels, levels[3].win[0]), SLAB, LANES), F32),
        ],
        [charges],
        flops=1 << 27,
    )
    band, lanes = call(
        functools.partial(bands_kernel, levels),
        [shape((16, 8 * TILE, 16 * TILE), BF16), shape((5 * LANES, 4 * LANES), BF16)],
        [taps.reshape(16, 17)],
        spaces={0: pltpu.SMEM},
        flops=1 << 26,
    )
    from_prev = shifted(up, "gx", 1)
    from_next = shifted(down, "gx", -1)
    far = far_pair(far, "gx")
    pieces = (x_prev, charges, x_next)
    y_prev = shifted(jnp.concatenate([x[:, -reach:] for x in pieces], 0), "gy", 1)
    y_next = shifted(jnp.concatenate([x[:, :reach] for x in pieces], 0), "gy", -1)

    y_slab = shape((slab_blocks(levels) * SLAB, LANES), BF16)
    r, up, down, far = call(
        functools.partial(rows_kernel, levels),
        [
            shape((sum(lv.full[0] * lv.rows for lv in coarse), LANES), F32),
            y_slab,
            y_slab,
            shape((far_groups(levels, levels[3].full[0]), SLAB, LANES), F32),
        ],
        [q, from_prev, from_next, *far],
        flops=1 << 25,
    )
    m_prev = shifted(up, "gy", 1)
    m_next = shifted(down, "gy", -1)
    far = far_pair(far, "gy")

    wide = jnp.concatenate([y_prev, jnp.concatenate(pieces, 0), y_next], 1)
    sides = call(
        halo_kernel,
        shape((2 * reach, wide.shape[0] * wide.shape[1]), BF16),
        [wide],
        flops=1 << 26,
    )
    halo = z_pair(sides, "gz")

    flat_rows = [lv.full[0] * lv.inp[1] for lv in coarse]
    slab_shapes = [
        (2 * coarse[0].sent, coarse[0].span),
        (2 * coarse[1].sent, 2 * (coarse[1].span + coarse[2].span)),
    ]
    groups = (coarse[:1], coarse[1:])
    (flat_one, slab_one), (flat_two, slab_two) = [
        call(
            functools.partial(lanes_kernel, levels, some, table),
            [shape((count, LANES), F32), shape(sizes, BF16)],
            [r, m_prev, m_next, table_array, *extra],
            scratch=[pltpu.VMEM((lv.span, LANES), F32) for lv in some],
            flops=1 << 26,
        )
        for some, count, sizes, extra in zip(
            groups, (flat_rows[0], flat_rows[1] + flat_rows[2]), slab_shapes, ([], far)
        )
    ]
    flats = (flat_one, flat_two)
    slab_one = z_pair(slab_one, "gz")
    slab_two = z_pair(slab_two, "gz")

    fine = call(
        functools.partial(fine_kernel, zero),
        shape(charges.shape, F32),
        [wide, halo, lanes, band],
        scratch=[
            pltpu.VMEM((*zero.inp, 4 * LANES), BF16),
            pltpu.VMEM((4, zero.out[1], zero.inp[0], LANES), BF16),
        ],
        flops=1 << 32,
        limit=20,
    )
    slab_one, fine = lax.optimization_barrier((slab_one, fine))

    def scratch(some):
        return [pltpu.VMEM((*lv.inp, 4 * LANES), BF16) for lv in some] + [
            pltpu.VMEM((4, lv.out[1], lv.inp[0], LANES), BF16) for lv in some
        ]

    middle = call(
        functools.partial(middle_kernel, levels, table),
        shape((*coarse[0].out, LANES), F32),
        [flats[0], slab_one, lanes, band, table_array],
        scratch=scratch(coarse[:1]),
        flops=1 << 31,
        limit=16,
    )
    return call(
        functools.partial(coarse_kernel, levels, table),
        shape(charges.shape, BF16),
        [flats[1], slab_two, lanes, band, table_array, middle, fine],
        scratch=scratch(coarse[1:])
        + [pltpu.VMEM((*lv.out, LANES), F32) for lv in coarse]
        + [pltpu.VMEM(charges.shape, BF16), pltpu.SemaphoreType.DMA((charges.shape[0] // 8,))],
        out_space=pl.ANY,
        flops=1 << 30,
        limit=16,
    )


def solution(mesh):
    return jax.shard_map(
        steps,
        mesh=mesh,
        in_specs=(P("gx", "gy", "gz"), P()),
        out_specs=P("gx", "gy", "gz"),
        check_vma=False,
    )
```
